256 devices in a mesh: dp: 16 (over z, x_lo), ctx: 16 (over x_hi, y, core).
Axes of the slice: x: 4 (x_hi: 2, x_lo: 2; x = x_hi * 2 + x_lo), y: 4, z: 8, core: 2. Of those that a mesh axis runs over, the one named last changes fastest.
Arguments:
- queries: bfloat16 [16, 4096, 2048], P('dp', 'ctx'), may hold values from -100 to 100
- keys: bfloat16 [16, 4096, 512], P('dp', 'ctx'), may hold values from -4 to 4
- values: bfloat16 [16, 4096, 512], P('dp', 'ctx'), may hold values from -6 to 6
- segments: int32 [16, 4096], P('dp', 'ctx'), may hold values from 0 to 7, never falling along the last dimension, each value on 1 to 2048 neighbouring positions
Outputs:
- attended: bfloat16 [16, 4096, 2048], P('dp', 'ctx')
The draws below stay inside these ranges and needn't reach their ends.
Inputs may be any that keep to these rules, and one draw needn't show every extreme that they name: `segments`: document numbers never fall along a packed batch, every one of the 8 documents is present, and each document has at most 2048 tokens; some document has exactly 2048.
All inputs are finite; a program needn't handle non-finite values.
Results may differ from the reference program's by a relative error of at most 0.0053.
Values may be sent and summed in bfloat16 or wider, within the bound.
A program may use at most 192 MiB of HBM per device.

```python
import math
import jax
import jax.numpy as jnp
import numpy as np
from jax import lax

HQ = 16
HK = 4
HD = 128
SEQ_COUNT = 8
TOKENS = 4096
MOST = 2048
N_DP = 16


def draw_pair(key):
    key_keys = jax.random.fold_in(key, 12)
    key_queries = jax.random.fold_in(key, 11)
    key_rows = jnp.clip(jax.random.normal(key_keys, (N_DP, TOKENS, HK * HD), jnp.float32), -4.0, 4.0)
    query_rows = jnp.clip(jax.random.normal(key_queries, (N_DP, TOKENS, HQ * HD), jnp.float32), -4.0, 4.0)
    return (query_rows, key_rows)


def draw_queries(key, part):
    return draw_pair(key)[0].astype(jnp.bfloat16)


def draw_keys(key, part):
    return draw_pair(key)[1].astype(jnp.bfloat16)


def level_of(rng, shape, cuts, smallest, largest):
    factor_of = 1.0
    for dim, blocks in cuts:
        draws = jax.random.uniform(jax.random.fold_in(jax.random.fold_in(rng, 6), dim), (blocks,), jnp.float32, smallest / len(cuts), largest / len(cuts))
        factor_of = factor_of * jnp.repeat(jnp.exp(draws), shape[dim] // blocks).reshape((-1,) + (1,) * (len(shape) - 1 - dim))
    return factor_of


def length_profile(number_of, total, bound, skew):
    loads = [(1 << 20) // math.isqrt(grade ** skew) + 1 for grade in range(2, number_of + 1)]
    spare, counts = total - bound - (number_of - 1), [1] * (number_of - 1)
    while spare > 0:
        movable = [i for i in range(number_of - 1) if counts[i] < bound]
        whole, left = sum([loads[i] for i in movable]), spare
        for i in movable:
            addition = min(bound - counts[i], max(1, left * loads[i] // whole), spare)
            counts[i] = counts[i] + addition
            spare = spare - addition
    return np.array([bound] + counts)


def ragged(own_key, number_of, total, reach, skew):
    if number_of == 2:
        one = jax.random.randint(own_key, (), max(1, total - reach), min(reach, total - 1) + 1)
        return jnp.stack([one, total - one])
    sizes = jnp.asarray(length_profile(number_of, total, reach, skew), jnp.int32)
    pairs = (number_of - 1) // 2
    giver, receiver = sizes[1:1 + 2 * pairs:2], sizes[2:2 + 2 * pairs:2]
    slack = jnp.minimum(giver - 1, reach - receiver)
    moved = jax.random.randint(jax.random.fold_in(own_key, 1), (pairs,), 0, 1 << 20) % (slack + 1)
    sizes = sizes.at[1:1 + 2 * pairs:2].set(giver - moved).at[2:2 + 2 * pairs:2].set(receiver + moved)
    return sizes[jax.random.permutation(jax.random.fold_in(own_key, 2), number_of)]


def scatter_about(stream_key, extent, scale, bound, cuts=(), held_as=jnp.bfloat16):
    entries = jax.random.normal(stream_key, extent, jnp.float32) * scale
    if len(cuts) > 0:
        entries = level_of(stream_key, extent, cuts, -0.22, 0.18) * entries
    return jnp.clip(entries, min=-bound, max=bound).astype(held_as)


def setup_inputs(seed: int = 0) -> dict:
    streams_of = jax.random.split(jax.random.key(seed), 5)
    queries = draw_queries(jax.random.fold_in(streams_of[4], 71), 0)
    keys = draw_keys(jax.random.fold_in(streams_of[4], 71), 0)
    values = scatter_about(streams_of[2], (N_DP, TOKENS, HK * HD), 1.0, 6.0, ((0, 16), (1, 16)))
    segments = jax.vmap(lambda own: jnp.searchsorted(jnp.cumsum(ragged(own, SEQ_COUNT, TOKENS, MOST, 2)), jnp.arange(TOKENS), side="right"))(jax.random.split(streams_of[3], N_DP)).reshape((N_DP, TOKENS)).astype(jnp.int32)
    return dict(queries=queries, keys=keys, values=values, segments=segments)


rope_theta = 500000.0

def rotate(values_in, positions, heads):
    rows = values_in.shape[0]
    half_dim = HD // 2
    split = values_in.astype(jnp.float32).reshape(rows, heads, HD)
    inv_freq = jnp.exp(-jnp.log(rope_theta) * 2.0 * jnp.arange(half_dim, dtype=jnp.float32) / HD)
    angles = positions.astype(jnp.float32)[:, None] * inv_freq[None, :]
    cosine_part = jnp.cos(angles)[:, None, :]
    sine_part = jnp.sin(angles)[:, None, :]
    first_half = split[..., :half_dim]
    second_half = split[..., half_dim:]
    turned = jnp.concatenate([first_half * cosine_part - second_half * sine_part, second_half * cosine_part + first_half * sine_part], axis=-1)
    return turned.reshape(rows, heads * HD).astype(jnp.bfloat16)

def doc_positions(seg_ids):
    index_all = jnp.arange(seg_ids.shape[0], dtype=jnp.int32)
    previous = jnp.concatenate([seg_ids[:1] - 1, seg_ids[:-1]])
    run_start = lax.cummax(jnp.where(seg_ids != previous, index_all, 0), axis=0)
    return index_all - run_start

def one_batch(inputs):
    query_rows, key_rows, value_rows, seg_ids = inputs
    positions = doc_positions(seg_ids)
    rot_q = rotate(query_rows, positions, HQ)
    rot_k = rotate(key_rows, positions, HK)
    block_rows = min(512, TOKENS)
    pieces = []
    for block_index in range(TOKENS // block_rows):
        q_lo = block_index * block_rows
        key_lo = max(0, q_lo - MOST)
        key_hi = q_lo + block_rows
        width = key_hi - key_lo
        query_heads = rot_q[q_lo:key_hi].astype(jnp.float32).reshape(block_rows, HK, HQ // HK, HD)
        key_heads = rot_k[key_lo:key_hi].astype(jnp.float32).reshape(width, HK, HD)
        value_heads = value_rows[key_lo:key_hi].astype(jnp.float32).reshape(width, HK, HD)
        q_index = q_lo + jnp.arange(block_rows, dtype=jnp.int32)
        k_index = key_lo + jnp.arange(width, dtype=jnp.int32)
        live_mask = (seg_ids[key_lo:key_hi][None, :] == seg_ids[q_lo:key_hi][:, None]) & (k_index[None, :] <= q_index[:, None])
        scores = jnp.einsum('thgd,shd->hgts', query_heads, key_heads) / jnp.sqrt(jnp.float32(HD))
        scores = jnp.where(live_mask, scores, jnp.float32(-1e+30))
        row_max = lax.optimization_barrier(jnp.max(scores, axis=-1, keepdims=True))
        weights = jnp.where(live_mask, jnp.exp(scores - row_max), jnp.float32(0.0))
        denom = lax.optimization_barrier(jnp.sum(weights, axis=-1))
        rounded = lax.optimization_barrier(weights.astype(jnp.bfloat16)).astype(jnp.float32)
        weighted = jnp.einsum('hgts,shd->thgd', rounded, value_heads)
        result = weighted / jnp.transpose(denom, (2, 0, 1))[..., None]
        pieces.append(result.reshape(block_rows, HQ * HD).astype(jnp.bfloat16))
    return jnp.concatenate(pieces, axis=0)

def reference(queries, keys, values, segments):
    attended = lax.map(one_batch, (queries, keys, values, segments))
    return attended
```

```python
import functools

import jax
import jax.numpy as jnp
from jax import lax
from jax.experimental import pallas as pl
from jax.experimental.pallas import tpu as pltpu
from jax.sharding import PartitionSpec as P

HQ = 16
HK = 4
HD = 128
GROUP = HQ // HK
HALF = HD // 2
ROWS = 256
NBACK = 8
THETA = 500000.0
DEAD = 1048576.0
MESH = pl.DeviceIdType.MESH


def cos_sin(angle):
    n = jnp.floor(angle * 0.6366197723675814 + 0.5)
    r = angle - n * 1.5703125
    r = r - n * 4.837512969970703125e-4
    r = r - n * 7.54978995489188216e-8
    z = r * r
    s = r + r * z * ((-1.9515295891e-4 * z + 8.3321608736e-3) * z - 1.6666654611e-1)
    c = 1.0 - 0.5 * z + z * z * (
        (2.443315711809948e-5 * z - 1.388731625493765e-3) * z + 4.166664568298827e-2
    )
    quarter = n.astype(jnp.int32) & 3
    odd = (quarter & 1) == 1
    cos_mag = jnp.where(odd, s, c)
    sin_mag = jnp.where(odd, c, s)
    cos = jnp.where((quarter == 1) | (quarter == 2), -cos_mag, cos_mag)
    sin = jnp.where(quarter >= 2, -sin_mag, sin_mag)
    return cos, sin


def rotated(block_t, cos, sin):
    wide = block_t.astype(jnp.float32)
    first, second = wide[:HALF], wide[HALF:]
    return jnp.concatenate(
        [first * cos - second * sin, second * cos + first * sin], axis=0
    ).astype(jnp.bfloat16)


def kernel(
    q_hbm, k_hbm, v_hbm, seg_hbm, out_ref,
    q_raw, k_raw, buf, segs, q_t, m_buf, e_buf, cos_buf, sin_buf, acc, top, total,
    in_sem, recv_sem, seg_recv, seg_send, y_send, x_send, d_send,
):
    d = lax.axis_index("ctx")
    core = lax.rem(d, 2)
    chip = lax.div(d, 2)
    col = lax.div(chip, 4)
    y = lax.rem(chip, 4)
    sibling = d + 1 - 2 * core
    scale = float(HD) ** -0.5 * 1.4426950408889634

    own = [
        pltpu.make_async_copy(seg_hbm, segs.at[0], in_sem.at[0]),
        pltpu.make_async_copy(k_hbm.at[0], k_raw, in_sem.at[1]),
        pltpu.make_async_copy(q_hbm.at[0], q_raw, in_sem.at[2]),
    ] + [
        pltpu.make_async_copy(
            v_hbm.at[0, :, pl.ds(h * HD, HD)], buf.at[0, HK + h], in_sem.at[3 + h]
        )
        for h in range(HK)
    ]
    for copy in own:
        copy.start()
    for j in range(1, NBACK + 1):
        segs[j] = jnp.full((1, ROWS), -1, jnp.int32)

    barrier = pltpu.get_barrier_semaphore()
    for k in range(1, 16):
        pl.semaphore_signal(
            barrier, inc=1, device_id={"ctx": lax.rem(d + k, 16)}, device_id_type=MESH
        )
    own[0].wait()
    for h in range(HK):
        own[3 + h].wait()
    pl.semaphore_wait(barrier, 15)

    def y_copy(src_slot, step, t):
        target = col * 8 + lax.rem(y + step, 4) * 2 + core
        return pltpu.make_async_remote_copy(
            buf.at[src_slot, t], buf.at[2 * step, t],
            y_send.at[step - 1, t], recv_sem.at[2 * step, t],
            device_id={"ctx": target}, device_id_type=MESH,
        )

    def x_copy(t):
        return pltpu.make_async_remote_copy(
            buf.at[0, t], buf.at[8, t], x_send.at[t], recv_sem.at[8, t],
            device_id={"ctx": lax.rem(d + 8, 16)}, device_id_type=MESH,
        )

    def d_copy(k, t):
        slot = 2 * k + 1 - 2 * core
        return pltpu.make_async_remote_copy(
            buf.at[2 * k, t], buf.at[slot, t], d_send.at[k, t], recv_sem.at[slot, t],
            device_id={"ctx": sibling}, device_id_type=MESH,
        )

    def seg_copy(j):
        return pltpu.make_async_remote_copy(
            segs.at[0], segs.at[j], seg_send.at[j], seg_recv.at[j],
            device_id={"ctx": lax.rem(d + j, 16)}, device_id_type=MESH,
        )

    def send_own(t, steps, others):
        for step in steps:
            @pl.when(y + step < 4)
            def _():
                y_copy(0, step, t).start()
        if others:
            @pl.when(chip < 4)
            def _():
                x_copy(t).start()

            @pl.when(core == 0)
            def _():
                d_copy_own(t).start()

    def d_copy_own(t):
        return pltpu.make_async_remote_copy(
            buf.at[0, t], buf.at[1, t], d_send.at[0, t], recv_sem.at[1, t],
            device_id={"ctx": sibling}, device_id_type=MESH,
        )

    for j in range(1, NBACK + 1):
        @pl.when(d + j < 16)
        def _():
            seg_copy(j).start()

    for h in range(HK):
        send_own(HK + h, (1, 3), True)

    for j in range(1, NBACK + 1):
        @pl.when(d >= j)
        def _():
            seg_copy(j).wait_recv()
    seg = segs[0]
    lane = lax.broadcasted_iota(jnp.int32, (1, ROWS), 1).astype(jnp.float32)
    first = jnp.min(seg.astype(jnp.float32), axis=1, keepdims=True)
    seg_f = seg.astype(jnp.float32)
    same = jnp.zeros((1, ROWS), jnp.float32)
    for j in range(1, NBACK + 1):
        same += jnp.where(segs[j].astype(jnp.float32) == first, 1.0, 0.0)
    carried = jnp.sum(same, axis=1, keepdims=True)
    start = jnp.zeros((1, ROWS), jnp.float32)
    for s in range(1, 8):
        before = jnp.sum(jnp.where(seg_f < float(s), 1.0, 0.0), axis=1, keepdims=True)
        start += jnp.where(seg_f == float(s), before, 0.0)
    pos = lane - start + jnp.where(seg_f == first, carried, 0.0)

    freq_index = lax.broadcasted_iota(jnp.int32, (HALF, ROWS), 0).astype(jnp.float32)
    inv_freq = jnp.exp(-jnp.log(jnp.float32(THETA)) * 2.0 * freq_index / HD)
    cos, sin = cos_sin(pos * inv_freq)
    cos_buf[...] = cos
    sin_buf[...] = sin

    own[1].wait()
    for h in range(HK):
        k_t = k_raw[:, h * HD : (h + 1) * HD].T
        buf[0, h] = rotated(k_t, cos, sin).T

    doc = lax.broadcasted_iota(jnp.int32, (HD, ROWS), 0)
    e_buf[...] = jnp.where(doc == seg, 1.0, 0.0).astype(jnp.bfloat16)

    def build_mask(j, carry):
        m_t = jnp.where(doc == segs[j], 0.0, -DEAD).astype(jnp.bfloat16)
        m_buf[j] = m_t.T
        return carry

    lax.fori_loop(0, NBACK + 1, build_mask, 0)

    for h in range(HK):
        send_own(h, (1, 3), True)
    for h in range(HK):
        send_own(HK + h, (2,), False)
        send_own(h, (2,), False)

    def wait_in(slot, t):
        pltpu.make_async_remote_copy(
            buf.at[slot, t], buf.at[slot, t], d_send.at[0, t], recv_sem.at[slot, t],
            device_id={"ctx": sibling}, device_id_type=MESH,
        ).wait_recv()

    def serve(k, t):
        @pl.when(chip >= k)
        def _():
            wait_in(2 * k, t)
            if k == 4:
                for step in (1, 3):
                    @pl.when(y + step >= 4)
                    def _():
                        y_copy(8, step, t).start()

                @pl.when(core == 1)
                def _():
                    d_copy(k, t).start()
            else:
                d_copy(k, t).start()

    def attend(slot, h, is_own):
        keys = jnp.concatenate([buf[slot, h], m_buf[slot]], axis=1)
        vals = buf[slot, HK + h].T
        for g in range(GROUP):
            n = h * GROUP + g
            quer = jnp.concatenate([q_t[n], e_buf[...]], axis=0)
            s = jnp.dot(keys, quer, preferred_element_type=jnp.float32)
            if is_own:
                later = lax.broadcasted_iota(jnp.int32, (ROWS, ROWS), 0) > (
                    lax.broadcasted_iota(jnp.int32, (ROWS, ROWS), 1)
                )
                s = jnp.where(later, -DEAD, s)
            peak = jnp.max(s, axis=0, keepdims=True)
            if not is_own:
                old = top[n]
                peak = jnp.maximum(old, peak)
                fade = jnp.exp2((old - peak) * scale)
            p = jnp.exp2((s - peak) * scale)
            part = jnp.sum(p, axis=0, keepdims=True)
            o = jnp.dot(vals, p.astype(jnp.bfloat16), preferred_element_type=jnp.float32)
            top[n] = peak
            if is_own:
                total[n] = part
                acc[n] = o
            else:
                total[n] = total[n] * fade + part
                acc[n] = acc[n] * fade + o

    own[2].wait()

    def own_step(h, carry):
        for g in range(GROUP):
            n = h * GROUP + g
            q_h = q_raw[:, pl.ds(pl.multiple_of(n * HD, HD), HD)]
            q_t[n] = rotated(q_h.T, cos_buf[...], sin_buf[...])
        for k in (4, 1, 3):
            serve(k, HK + h)
        attend(0, h, True)
        return carry

    lax.fori_loop(0, HK, own_step, 0)

    def near_step(h, carry):
        for k in (4, 1, 3):
            serve(k, h)

        @pl.when(core == 1)
        def _():
            wait_in(1, HK + h)
            wait_in(1, h)
            attend(1, h, False)

        for k in (4, 1, 3):
            @pl.when(chip >= k)
            def _():
                attend(2 * k, h, False)
        for k in (4, 1, 3):
            @pl.when((chip >= k) & (2 * k - 1 + 2 * core < 9))
            def _():
                slot = 2 * k - 1 + 2 * core
                wait_in(slot, HK + h)
                wait_in(slot, h)
                attend(slot, h, False)
        return carry

    def hand_far(t, carry):
        @pl.when((col == 1) & (y + 2 >= 4))
        def _():
            y_copy(8, 2, t).start()
        return carry

    def near_all(h, carry):
        near_step(h, carry)

        @pl.when(h == HK - 1)
        def _():
            lax.fori_loop(0, 2 * HK, hand_far, 0)
        return carry

    lax.fori_loop(0, HK, near_all, 0)

    def far_step(h, carry):
        serve(2, HK + h)
        serve(2, h)

        @pl.when(chip >= 2)
        def _():
            attend(4, h, False)
            slot = 3 + 2 * core
            wait_in(slot, HK + h)
            wait_in(slot, h)
            attend(slot, h, False)

        for g in range(GROUP):
            n = h * GROUP + g
            o = (acc[n] / total[n]).T
            out_ref[0, :, pl.ds(pl.multiple_of(n * HD, HD), HD)] = o.astype(jnp.bfloat16)
        return carry

    lax.fori_loop(0, HK, far_step, 0)

    for j in range(1, NBACK + 1):
        @pl.when(d + j < 16)
        def _():
            seg_copy(j).wait_send()

    def drain(t, carry):
        for step in (1, 2, 3):
            @pl.when((col == 1) | (y + step < 4))
            def _():
                y_copy(0, step, t).wait_send()

        @pl.when(chip < 4)
        def _():
            x_copy(t).wait_send()

        @pl.when(core == 0)
        def _():
            d_copy_own(t).wait_send()

        for k in (1, 2, 3):
            @pl.when(chip >= k)
            def _():
                d_copy(k, t).wait_send()

        @pl.when((chip >= 4) & (core == 1))
        def _():
            d_copy(4, t).wait_send()
        return carry

    lax.fori_loop(0, 2 * HK, drain, 0)


def body(queries, keys, values, segments):
    hbm = pl.BlockSpec(memory_space=pl.ANY)
    return pl.pallas_call(
        kernel,
        out_shape=jax.ShapeDtypeStruct((1, ROWS, HQ * HD), jnp.bfloat16),
        in_specs=[hbm] * 4,
        out_specs=pl.BlockSpec(memory_space=pltpu.VMEM),
        scratch_shapes=[
            pltpu.VMEM((ROWS, HQ * HD), jnp.bfloat16),
            pltpu.VMEM((ROWS, HK * HD), jnp.bfloat16),
            pltpu.VMEM((NBACK + 1, 2 * HK, ROWS, HD), jnp.bfloat16),
            pltpu.VMEM((NBACK + 1, 1, ROWS), jnp.int32),
            pltpu.VMEM((HQ, HD, ROWS), jnp.bfloat16),
            pltpu.VMEM((NBACK + 1, ROWS, HD), jnp.bfloat16),
            pltpu.VMEM((HD, ROWS), jnp.bfloat16),
            pltpu.VMEM((HALF, ROWS), jnp.float32),
            pltpu.VMEM((HALF, ROWS), jnp.float32),
            pltpu.VMEM((HQ, HD, ROWS), jnp.float32),
            pltpu.VMEM((HQ, 1, ROWS), jnp.float32),
            pltpu.VMEM((HQ, 1, ROWS), jnp.float32),
            pltpu.SemaphoreType.DMA((7,)),
            pltpu.SemaphoreType.DMA((NBACK + 1, 2 * HK)),
            pltpu.SemaphoreType.DMA((NBACK + 1,)),
            pltpu.SemaphoreType.DMA((NBACK + 1,)),
            pltpu.SemaphoreType.DMA((3, 2 * HK)),
            pltpu.SemaphoreType.DMA((2 * HK,)),
            pltpu.SemaphoreType.DMA((5, 2 * HK)),
        ],
        compiler_params=pltpu.CompilerParams(collective_id=0, has_side_effects=True),
    )(queries, keys, values, segments)


def solution(mesh):
    placed = (P("dp", "ctx", None), P("dp", "ctx", None), P("dp", "ctx", None), P("dp", "ctx"))
    return jax.shard_map(
        body, mesh=mesh, in_specs=placed, out_specs=P("dp", "ctx", None), check_vma=False
    )
```

```python
import jax
import jax.numpy as jnp
from jax import lax
from jax.experimental import pallas as pl
from jax.experimental.pallas import tpu as pltpu
from jax.sharding import PartitionSpec as P

HQ = 16
HK = 4
HD = 128
GROUP = HQ // HK
HALF = HD // 2
ROWS = 256
NBACK = 8
THETA = 500000.0
DEAD = 1048576.0
MESH = pl.DeviceIdType.MESH


def cos_sin(angle):
    n = jnp.floor(angle * 0.6366197723675814 + 0.5)
    r = angle - n * 1.5703125
    r = r - n * 4.837512969970703125e-4
    r = r - n * 7.54978995489188216e-8
    z = r * r
    s = r + r * z * ((-1.9515295891e-4 * z + 8.3321608736e-3) * z - 1.6666654611e-1)
    c = 1.0 - 0.5 * z + z * z * (
        (2.443315711809948e-5 * z - 1.388731625493765e-3) * z + 4.166664568298827e-2
    )
    quarter = n.astype(jnp.int32) & 3
    odd = (quarter & 1) == 1
    cos_mag = jnp.where(odd, s, c)
    sin_mag = jnp.where(odd, c, s)
    cos = jnp.where((quarter == 1) | (quarter == 2), -cos_mag, cos_mag)
    sin = jnp.where(quarter >= 2, -sin_mag, sin_mag)
    return cos, sin


def rotated(block_t, cos, sin):
    wide = block_t.astype(jnp.float32)
    first, second = wide[:HALF], wide[HALF:]
    return jnp.concatenate(
        [first * cos - second * sin, second * cos + first * sin], axis=0
    ).astype(jnp.bfloat16)


def kernel(
    q_hbm, k_hbm, v_hbm, seg_hbm, out_ref,
    q_raw, k_raw, buf, segs, q_t, m_buf, e_buf, cos_buf, sin_buf, acc, top, total, s_even, s_odd, p_even, p_odd,
    in_sem, recv_sem, seg_recv, seg_send, y_send, x_send, d_send,
):
    d = lax.axis_index("ctx")
    core = lax.rem(d, 2)
    chip = lax.div(d, 2)
    col = lax.div(chip, 4)
    y = lax.rem(chip, 4)
    sibling = d + 1 - 2 * core
    s_buf, p_buf = (s_even, s_odd), (p_even, p_odd)
    scale = float(HD) ** -0.5 * 1.4426950408889634

    own = [
        pltpu.make_async_copy(seg_hbm, segs.at[0], in_sem.at[0]),
        pltpu.make_async_copy(k_hbm.at[0], k_raw, in_sem.at[1]),
        pltpu.make_async_copy(q_hbm.at[0], q_raw, in_sem.at[2]),
    ] + [
        pltpu.make_async_copy(
            v_hbm.at[0, :, pl.ds(h * HD, HD)], buf.at[0, HK + h], in_sem.at[3 + h]
        )
        for h in range(HK)
    ]
    for copy in own:
        copy.start()
    for j in range(1, NBACK + 1):
        segs[j] = jnp.full((1, ROWS), -1, jnp.int32)

    barrier = pltpu.get_barrier_semaphore()
    for k in range(1, 16):
        pl.semaphore_signal(
            barrier, inc=1, device_id={"ctx": lax.rem(d + k, 16)}, device_id_type=MESH
        )
    own[0].wait()
    for h in range(HK):
        own[3 + h].wait()
    pl.semaphore_wait(barrier, 15)

    def y_copy(src_slot, step, t):
        target = col * 8 + lax.rem(y + step, 4) * 2 + core
        return pltpu.make_async_remote_copy(
            buf.at[src_slot, t], buf.at[2 * step, t],
            y_send.at[step - 1, t], recv_sem.at[2 * step, t],
            device_id={"ctx": target}, device_id_type=MESH,
        )

    def x_copy(t):
        return pltpu.make_async_remote_copy(
            buf.at[0, t], buf.at[8, t], x_send.at[t], recv_sem.at[8, t],
            device_id={"ctx": lax.rem(d + 8, 16)}, device_id_type=MESH,
        )

    def d_copy(k, t):
        slot = 2 * k + 1 - 2 * core
        return pltpu.make_async_remote_copy(
            buf.at[2 * k, t], buf.at[slot, t], d_send.at[k, t], recv_sem.at[slot, t],
            device_id={"ctx": sibling}, device_id_type=MESH,
        )

    def seg_copy(j):
        return pltpu.make_async_remote_copy(
            segs.at[0], segs.at[j], seg_send.at[j], seg_recv.at[j],
            device_id={"ctx": lax.rem(d + j, 16)}, device_id_type=MESH,
        )

    def send_own(t, steps, others):
        for step in steps:
            @pl.when(y + step < 4)
            def _():
                y_copy(0, step, t).start()
        if others:
            @pl.when(chip < 4)
            def _():
                x_copy(t).start()

            @pl.when(core == 0)
            def _():
                d_copy_own(t).start()

    def d_copy_own(t):
        return pltpu.make_async_remote_copy(
            buf.at[0, t], buf.at[1, t], d_send.at[0, t], recv_sem.at[1, t],
            device_id={"ctx": sibling}, device_id_type=MESH,
        )

    for j in range(1, NBACK + 1):
        @pl.when(d + j < 16)
        def _():
            seg_copy(j).start()

    for h in range(HK):
        send_own(HK + h, (1, 3), True)

    for j in range(1, NBACK + 1):
        @pl.when(d >= j)
        def _():
            seg_copy(j).wait_recv()
    seg = segs[0]
    lane = lax.broadcasted_iota(jnp.int32, (1, ROWS), 1).astype(jnp.float32)
    first = jnp.min(seg.astype(jnp.float32), axis=1, keepdims=True)
    seg_f = seg.astype(jnp.float32)
    same = jnp.zeros((1, ROWS), jnp.float32)
    for j in range(1, NBACK + 1):
        same += jnp.where(segs[j].astype(jnp.float32) == first, 1.0, 0.0)
    carried = jnp.sum(same, axis=1, keepdims=True)
    start = jnp.zeros((1, ROWS), jnp.float32)
    for s in range(1, 8):
        before = jnp.sum(jnp.where(seg_f < float(s), 1.0, 0.0), axis=1, keepdims=True)
        start += jnp.where(seg_f == float(s), before, 0.0)
    pos = lane - start + jnp.where(seg_f == first, carried, 0.0)

    freq_index = lax.broadcasted_iota(jnp.int32, (HALF, ROWS), 0).astype(jnp.float32)
    inv_freq = jnp.exp(-jnp.log(jnp.float32(THETA)) * 2.0 * freq_index / HD)
    cos, sin = cos_sin(pos * inv_freq)
    cos_buf[...] = cos
    sin_buf[...] = sin

    own[1].wait()
    for h in range(HK):
        k_t = k_raw[:, h * HD : (h + 1) * HD].T
        buf[0, h] = rotated(k_t, cos, sin).T

    doc = lax.broadcasted_iota(jnp.int32, (HD, ROWS), 0)
    e_buf[...] = jnp.where(doc == seg, 1.0, 0.0).astype(jnp.bfloat16)

    def build_mask(j, carry):
        m_t = jnp.where(doc == segs[j], 0.0, -DEAD).astype(jnp.bfloat16)
        m_buf[j] = m_t.T
        return carry

    lax.fori_loop(0, NBACK + 1, build_mask, 0)

    for h in range(HK):
        send_own(h, (1, 3), True)
    for h in range(HK):
        send_own(HK + h, (2,), False)
        send_own(h, (2,), False)

    def wait_in(slot, t):
        pltpu.make_async_remote_copy(
            buf.at[slot, t], buf.at[slot, t], d_send.at[0, t], recv_sem.at[slot, t],
            device_id={"ctx": sibling}, device_id_type=MESH,
        ).wait_recv()

    def serve(k, t, far_too=None):
        @pl.when(chip >= k)
        def _():
            wait_in(2 * k, t)
            if k == 4:
                for step in (1, 3):
                    @pl.when(y + step >= 4)
                    def _():
                        y_copy(8, step, t).start()
                if far_too is not None:
                    @pl.when(y >= 2)
                    def _():
                        for u in far_too:
                            y_copy(8, 2, u).start()

                @pl.when(core == 1)
                def _():
                    d_copy(k, t).start()
            else:
                d_copy(k, t).start()

    def serve_near(t, far_too=None):
        for k in (4, 1, 3):
            serve(k, t, far_too)

    def serve_far(h):
        serve(2, HK + h)
        serve(2, h)

    def unit(slots, h, is_own=False):
        width = len(slots) * ROWS

        def scores(g):
            n = h * GROUP + g
            quer = jnp.concatenate([q_t[n], e_buf[...]], axis=0)
            peak = None if is_own else top[n]
            for i, slot in enumerate(slots):
                keys = jnp.concatenate([buf[slot, h], m_buf[slot]], axis=1)
                s = jnp.dot(keys, quer, preferred_element_type=jnp.float32)
                if is_own and i == 0:
                    later = lax.broadcasted_iota(jnp.int32, (ROWS, ROWS), 0) > (
                        lax.broadcasted_iota(jnp.int32, (ROWS, ROWS), 1)
                    )
                    s = jnp.where(later, -DEAD, s)
                s_buf[g % 2][pl.ds(i * ROWS, ROWS)] = s
                high = jnp.max(s, axis=0, keepdims=True)
                peak = high if peak is None else jnp.maximum(peak, high)
            return peak

        def weigh(g, peak):
            n = h * GROUP + g
            fade = None if is_own else jnp.exp2((top[n] - peak) * scale)
            top[n] = peak
            for i in range(len(slots)):
                p = jnp.exp2((s_buf[g % 2][pl.ds(i * ROWS, ROWS)] - peak) * scale)
                p_buf[g % 2][pl.ds(i * ROWS, ROWS)] = p.astype(jnp.bfloat16)
            return fade

        def add_up(g, fade):
            n = h * GROUP + g
            vals = jnp.concatenate([buf[slot, HK + h].T for slot in slots], axis=1)
            vals = jnp.concatenate([vals, jnp.ones((16, width), jnp.bfloat16)], axis=0)
            o = jnp.dot(vals, p_buf[g % 2][pl.ds(0, width)], preferred_element_type=jnp.float32)
            if is_own:
                acc[n] = o[:HD]
                total[n] = o[HD : HD + 1]
            else:
                acc[n] = acc[n] * fade + o[:HD]
                total[n] = total[n] * fade + o[HD : HD + 1]

        peaks, fades = {}, {}
        for i in range(GROUP + 2):
            if i < GROUP:
                peaks[i] = scores(i)
            if 0 <= i - 2 < GROUP:
                add_up(i - 2, fades[i - 2])
            if 0 <= i - 1 < GROUP:
                fades[i - 1] = weigh(i - 1, peaks[i - 1])

    def pair(k, h):
        @pl.when(chip >= k)
        def _():
            slot = 2 * k - 1 + 2 * core

            @pl.when(slot < 9)
            def _():
                wait_in(slot, HK + h)
                wait_in(slot, h)
                unit([2 * k, slot], h)

            @pl.when(slot >= 9)
            def _():
                unit([2 * k], h)

    own[2].wait()

    def own_step(h, carry):
        serve_near(HK + h)
        for g in range(GROUP):
            n = h * GROUP + g
            q_h = q_raw[:, pl.ds(pl.multiple_of(n * HD, HD), HD)]
            q_t[n] = rotated(q_h.T, cos_buf[...], sin_buf[...])

        @pl.when(core == 0)
        def _():
            unit([0], h, True)

        @pl.when(core == 1)
        def _():
            wait_in(1, HK + h)
            wait_in(1, h)
            unit([0, 1], h, True)
        return carry

    lax.fori_loop(0, HK, own_step, 0)
    serve_near(0, (HK, 0))

    def near_step(h, carry):
        def near_unit(i, inner):
            pair(jnp.where(i == 0, 4, 2 * i - 1), h)

            @pl.when(h == 0)
            def _():
                serve_near(i + 1, (HK + i + 1, i + 1))

            @pl.when((h > 0) & (i == 2))
            def _():
                serve_far(h - 1)
            return inner

        return lax.fori_loop(0, 3, near_unit, carry)

    lax.fori_loop(0, HK, near_step, 0)

    def far_step(h, carry):
        @pl.when(h == HK - 1)
        def _():
            serve_far(h)

        pair(2, h)
        for g in range(GROUP):
            n = h * GROUP + g
            o = (acc[n] / total[n]).T
            out_ref[0, :, pl.ds(pl.multiple_of(n * HD, HD), HD)] = o.astype(jnp.bfloat16)
        return carry

    lax.fori_loop(0, HK, far_step, 0)

    for j in range(1, NBACK + 1):
        @pl.when(d + j < 16)
        def _():
            seg_copy(j).wait_send()

    def drain(t, carry):
        for step in (1, 2, 3):
            @pl.when((col == 1) | (y + step < 4))
            def _():
                y_copy(0, step, t).wait_send()

        @pl.when(chip < 4)
        def _():
            x_copy(t).wait_send()

        @pl.when(core == 0)
        def _():
            d_copy_own(t).wait_send()

        for k in (1, 2, 3):
            @pl.when(chip >= k)
            def _():
                d_copy(k, t).wait_send()

        @pl.when((chip >= 4) & (core == 1))
        def _():
            d_copy(4, t).wait_send()
        return carry

    lax.fori_loop(0, 2 * HK, drain, 0)


def body(queries, keys, values, segments):
    hbm = pl.BlockSpec(memory_space=pl.ANY)
    return pl.pallas_call(
        kernel,
        out_shape=jax.ShapeDtypeStruct((1, ROWS, HQ * HD), jnp.bfloat16),
        in_specs=[hbm] * 4,
        out_specs=pl.BlockSpec(memory_space=pltpu.VMEM),
        scratch_shapes=[
            pltpu.VMEM((ROWS, HQ * HD), jnp.bfloat16),
            pltpu.VMEM((ROWS, HK * HD), jnp.bfloat16),
            pltpu.VMEM((NBACK + 1, 2 * HK, ROWS, HD), jnp.bfloat16),
            pltpu.VMEM((NBACK + 1, 1, ROWS), jnp.int32),
            pltpu.VMEM((HQ, HD, ROWS), jnp.bfloat16),
            pltpu.VMEM((NBACK + 1, ROWS, HD), jnp.bfloat16),
            pltpu.VMEM((HD, ROWS), jnp.bfloat16),
            pltpu.VMEM((HALF, ROWS), jnp.float32),
            pltpu.VMEM((HALF, ROWS), jnp.float32),
            pltpu.VMEM((HQ, HD, ROWS), jnp.float32),
            pltpu.VMEM((HQ, 1, ROWS), jnp.float32),
            pltpu.VMEM((HQ, 1, ROWS), jnp.float32),
            pltpu.VMEM((2 * ROWS, ROWS), jnp.float32),
            pltpu.VMEM((2 * ROWS, ROWS), jnp.float32),
            pltpu.VMEM((2 * ROWS, ROWS), jnp.bfloat16),
            pltpu.VMEM((2 * ROWS, ROWS), jnp.bfloat16),
            pltpu.SemaphoreType.DMA((7,)),
            pltpu.SemaphoreType.DMA((NBACK + 1, 2 * HK)),
            pltpu.SemaphoreType.DMA((NBACK + 1,)),
            pltpu.SemaphoreType.DMA((NBACK + 1,)),
            pltpu.SemaphoreType.DMA((3, 2 * HK)),
            pltpu.SemaphoreType.DMA((2 * HK,)),
            pltpu.SemaphoreType.DMA((5, 2 * HK)),
        ],
        compiler_params=pltpu.CompilerParams(collective_id=0, has_side_effects=True),
    )(queries, keys, values, segments)


def solution(mesh):
    placed = (P("dp", "ctx", None), P("dp", "ctx", None), P("dp", "ctx", None), P("dp", "ctx"))
    return jax.shard_map(
        body, mesh=mesh, in_specs=placed, out_specs=P("dp", "ctx", None), check_vma=False
    )
```

```python
import jax
import jax.numpy as jnp
from jax import lax
from jax.experimental import pallas as pl
from jax.experimental.pallas import tpu as pltpu
from jax.sharding import PartitionSpec as P

HQ = 16
HK = 4
HD = 128
GROUP = HQ // HK
HALF = HD // 2
ROWS = 256
NBACK = 8
SPARE = 9
THETA = 500000.0
DEAD = 1048576.0
MESH = pl.DeviceIdType.MESH


def cos_sin(angle):
    n = jnp.floor(angle * 0.6366197723675814 + 0.5)
    r = angle - n * 1.5703125
    r = r - n * 4.837512969970703125e-4
    r = r - n * 7.54978995489188216e-8
    z = r * r
    s = r + r * z * ((-1.9515295891e-4 * z + 8.3321608736e-3) * z - 1.6666654611e-1)
    c = 1.0 - 0.5 * z + z * z * (
        (2.443315711809948e-5 * z - 1.388731625493765e-3) * z + 4.166664568298827e-2
    )
    quarter = n.astype(jnp.int32) & 3
    odd = (quarter & 1) == 1
    cos_mag = jnp.where(odd, s, c)
    sin_mag = jnp.where(odd, c, s)
    cos = jnp.where((quarter == 1) | (quarter == 2), -cos_mag, cos_mag)
    sin = jnp.where(quarter >= 2, -sin_mag, sin_mag)
    return cos, sin


def rotated(block_t, cos, sin):
    wide = block_t.astype(jnp.float32)
    first, second = wide[:HALF], wide[HALF:]
    return jnp.concatenate(
        [first * cos - second * sin, second * cos + first * sin], axis=0
    ).astype(jnp.bfloat16)


def kernel(
    q_hbm, k_hbm, v_hbm, seg_hbm, out_ref,
    q_raw, k_raw, buf, segs, q_t, m_buf, e_buf, cos_buf, sin_buf, acc, top, total, s_even, s_odd, p_even, p_odd,
    in_sem, recv_sem, seg_recv, seg_send, y_send, x_send, d_send,
    r_send, f_send, s_send,
):
    d = lax.axis_index("ctx")
    core = lax.rem(d, 2)
    chip = lax.div(d, 2)
    col = lax.div(chip, 4)
    y = lax.rem(chip, 4)
    sibling = d + 1 - 2 * core
    s_buf, p_buf = (s_even, s_odd), (p_even, p_odd)
    scale = float(HD) ** -0.5 * 1.4426950408889634

    own = [
        pltpu.make_async_copy(seg_hbm, segs.at[0], in_sem.at[0]),
        pltpu.make_async_copy(k_hbm.at[0], k_raw, in_sem.at[1]),
        pltpu.make_async_copy(q_hbm.at[0], q_raw, in_sem.at[2]),
    ] + [
        pltpu.make_async_copy(
            v_hbm.at[0, :, pl.ds(h * HD, HD)], buf.at[0, HK + h], in_sem.at[3 + h]
        )
        for h in range(HK)
    ]
    for copy in own:
        copy.start()
    for j in range(1, NBACK + 1):
        segs[j] = jnp.full((1, ROWS), -1, jnp.int32)

    barrier = pltpu.get_barrier_semaphore()
    for k in range(1, 16):
        pl.semaphore_signal(
            barrier, inc=1, device_id={"ctx": lax.rem(d + k, 16)}, device_id_type=MESH
        )
    own[0].wait()
    for h in range(HK):
        own[3 + h].wait()
    pl.semaphore_wait(barrier, 15)

    def copy_to(src_slot, dst_slot, target, sem, t):
        return pltpu.make_async_remote_copy(
            buf.at[src_slot, t], buf.at[dst_slot, t], sem, recv_sem.at[dst_slot, t],
            device_id={"ctx": target}, device_id_type=MESH,
        )

    def ring(step):
        return col * 8 + lax.rem(y + step, 4) * 2 + core

    across = lax.rem(d + 8, 16)

    def y_copy(src_slot, step, t):
        return copy_to(src_slot, 2 * step, ring(step), y_send.at[step // 2, t], t)

    def x_copy(t):
        return copy_to(0, 8, across, x_send.at[t], t)

    def relay_up(t):
        return copy_to(2, 4, ring(1), r_send.at[t], t)

    def relay_down(t):
        return copy_to(6, 4, ring(3), r_send.at[t], t)

    def direct_far(t):
        return copy_to(0, 4, ring(2), f_send.at[t], t)

    def park(t):
        return copy_to(0, SPARE, ring(2), f_send.at[t], t)

    def cross_spare(t):
        return copy_to(SPARE, 4, across, s_send.at[t], t)

    def cross_park(t):
        return copy_to(2, SPARE, across, s_send.at[t], t)

    def wrap_spare(t):
        return copy_to(SPARE, 4, ring(1), s_send.at[t], t)

    def d_copy(k, t):
        return copy_to(2 * k, 2 * k + 1 - 2 * core, sibling, d_send.at[k, t], t)

    def d_copy_own(t):
        return copy_to(0, 1, sibling, d_send.at[0, t], t)

    def seg_copy(j):
        return pltpu.make_async_remote_copy(
            segs.at[0], segs.at[j], seg_send.at[j], seg_recv.at[j],
            device_id={"ctx": lax.rem(d + j, 16)}, device_id_type=MESH,
        )

    def send_own(t):
        for step in (1, 3):
            @pl.when(y + step < 4)
            def _():
                y_copy(0, step, t).start()

        @pl.when(col == 0)
        def _():
            x_copy(t).start()

        @pl.when(core == 0)
        def _():
            d_copy_own(t).start()

    def send_far(h):
        for t in (HK + h, h):
            if h >= 2:
                @pl.when(y == 1)
                def _():
                    direct_far(t).start()

            @pl.when((col == 0) & (y == (2 if h < 2 else 3)))
            def _():
                park(t).start()

    for j in range(1, NBACK + 1):
        @pl.when(d + j < 16)
        def _():
            seg_copy(j).start()

    for h in range(HK):
        send_own(HK + h)

    for j in range(1, NBACK + 1):
        @pl.when(d >= j)
        def _():
            seg_copy(j).wait_recv()
    seg = segs[0]
    lane = lax.broadcasted_iota(jnp.int32, (1, ROWS), 1).astype(jnp.float32)
    first = jnp.min(seg.astype(jnp.float32), axis=1, keepdims=True)
    seg_f = seg.astype(jnp.float32)
    same = jnp.zeros((1, ROWS), jnp.float32)
    for j in range(1, NBACK + 1):
        same += jnp.where(segs[j].astype(jnp.float32) == first, 1.0, 0.0)
    carried = jnp.sum(same, axis=1, keepdims=True)
    start = jnp.zeros((1, ROWS), jnp.float32)
    for s in range(1, 8):
        before = jnp.sum(jnp.where(seg_f < float(s), 1.0, 0.0), axis=1, keepdims=True)
        start += jnp.where(seg_f == float(s), before, 0.0)
    pos = lane - start + jnp.where(seg_f == first, carried, 0.0)

    freq_index = lax.broadcasted_iota(jnp.int32, (HALF, ROWS), 0).astype(jnp.float32)
    inv_freq = jnp.exp(-jnp.log(jnp.float32(THETA)) * 2.0 * freq_index / HD)
    cos, sin = cos_sin(pos * inv_freq)
    cos_buf[...] = cos
    sin_buf[...] = sin

    own[1].wait()
    for h in range(HK):
        k_t = k_raw[:, h * HD : (h + 1) * HD].T
        buf[0, h] = rotated(k_t, cos, sin).T

    doc = lax.broadcasted_iota(jnp.int32, (HD, ROWS), 0)
    e_buf[...] = jnp.where(doc == seg, 1.0, 0.0).astype(jnp.bfloat16)

    def build_mask(j, carry):
        m_t = jnp.where(doc == segs[j], 0.0, -DEAD).astype(jnp.bfloat16)
        m_buf[j] = m_t.T
        return carry

    lax.fori_loop(0, NBACK + 1, build_mask, 0)

    for h in range(HK):
        send_own(h)
    for h in range(HK):
        send_far(h)

    def wait_in(slot, t):
        pltpu.make_async_remote_copy(
            buf.at[slot, t], buf.at[slot, t], d_send.at[0, t], recv_sem.at[slot, t],
            device_id={"ctx": sibling}, device_id_type=MESH,
        ).wait_recv()

    def serve(k, h, kind):
        t = h + kind

        @pl.when(chip >= k)
        def _():
            wait_in(2 * k, t)
            if k == 4:
                for step in (1, 3):
                    @pl.when(y + step >= 4)
                    def _():
                        y_copy(8, step, t).start()

                @pl.when(core == 1)
                def _():
                    d_copy(k, t).start()
                return
            if k == 1:
                @pl.when((h < 2) & (y < 3))
                def _():
                    relay_up(t).start()

                @pl.when((h >= 2) & (col == 0) & (y == 3))
                def _():
                    cross_park(t).start()
            if k == 3:
                @pl.when((h >= 2) & (y == 3))
                def _():
                    relay_down(t).start()
            d_copy(k, t).start()

    def serve_spare(h, kind):
        t = h + kind

        @pl.when((col == 0) & (y == jnp.where(h < 2, 0, 1)))
        def _():
            wait_in(SPARE, t)
            cross_spare(t).start()

        @pl.when((col == 1) & (y == 3) & (h >= 2))
        def _():
            wait_in(SPARE, t)
            wrap_spare(t).start()

    def unit(slots, h, is_own=False):
        width = len(slots) * ROWS

        def scores(g):
            n = h * GROUP + g
            quer = jnp.concatenate([q_t[n], e_buf[...]], axis=0)
            peak = None if is_own else top[n]
            for i, slot in enumerate(slots):
                keys = jnp.concatenate([buf[slot, h], m_buf[slot]], axis=1)
                s = jnp.dot(keys, quer, preferred_element_type=jnp.float32)
                if is_own and i == 0:
                    later = lax.broadcasted_iota(jnp.int32, (ROWS, ROWS), 0) > (
                        lax.broadcasted_iota(jnp.int32, (ROWS, ROWS), 1)
                    )
                    s = jnp.where(later, -DEAD, s)
                s_buf[g % 2][pl.ds(i * ROWS, ROWS)] = s
                high = jnp.max(s, axis=0, keepdims=True)
                peak = high if peak is None else jnp.maximum(peak, high)
            return peak

        def weigh(g, peak):
            n = h * GROUP + g
            fade = None if is_own else jnp.exp2((top[n] - peak) * scale)
            top[n] = peak
            for i in range(len(slots)):
                p = jnp.exp2((s_buf[g % 2][pl.ds(i * ROWS, ROWS)] - peak) * scale)
                p_buf[g % 2][pl.ds(i * ROWS, ROWS)] = p.astype(jnp.bfloat16)
            return fade

        def add_up(g, fade):
            n = h * GROUP + g
            vals = jnp.concatenate([buf[slot, HK + h].T for slot in slots], axis=1)
            vals = jnp.concatenate([vals, jnp.ones((16, width), jnp.bfloat16)], axis=0)
            o = jnp.dot(vals, p_buf[g % 2][pl.ds(0, width)], preferred_element_type=jnp.float32)
            if is_own:
                acc[n] = o[:HD]
                total[n] = o[HD : HD + 1]
            else:
                acc[n] = acc[n] * fade + o[:HD]
                total[n] = total[n] * fade + o[HD : HD + 1]

        peaks, fades = {}, {}
        for i in range(GROUP + 2):
            if i < GROUP:
                peaks[i] = scores(i)
            if 0 <= i - 2 < GROUP:
                add_up(i - 2, fades[i - 2])
            if 0 <= i - 1 < GROUP:
                fades[i - 1] = weigh(i - 1, peaks[i - 1])

    def pair(k, h):
        @pl.when(chip >= k)
        def _():
            slot = 2 * k - 1 + 2 * core

            @pl.when(slot < 9)
            def _():
                wait_in(slot, HK + h)
                wait_in(slot, h)
                unit([2 * k, slot], h)

            @pl.when(slot >= 9)
            def _():
                unit([2 * k], h)

    own[2].wait()

    def own_step(h, carry):
        serve(4, h, HK)
        for g in range(GROUP):
            n = h * GROUP + g
            q_h = q_raw[:, pl.ds(pl.multiple_of(n * HD, HD), HD)]
            q_t[n] = rotated(q_h.T, cos_buf[...], sin_buf[...])
        serve(1, h, HK)
        serve(3, h, HK)

        @pl.when(core == 0)
        def _():
            unit([0], h, True)

        @pl.when(core == 1)
        def _():
            wait_in(1, HK + h)
            wait_in(1, h)
            unit([0, 1], h, True)
        return carry

    lax.fori_loop(0, HK, own_step, 0)

    serve(4, 0, 0)
    serve(1, 0, 0)
    serve(3, 0, 0)

    def spare_values(h, carry):
        serve_spare(h, HK)
        return carry

    def near_step(h, carry):
        def near_unit(i, inner):
            pair(jnp.where(i == 0, 4, 2 * i - 1), h)

            @pl.when(h == 0)
            def _():
                serve(4, i + 1, 0)
                serve(1, i + 1, 0)
                serve(3, i + 1, 0)

            @pl.when((h == 0) & (i == 0))
            def _():
                lax.fori_loop(0, HK, spare_values, 0)

            @pl.when(h == 1)
            def _():
                serve_spare(i, 0)
                serve(2, i, HK)

            @pl.when((h == 1) & (i == 2))
            def _():
                serve_spare(3, 0)
                serve(2, 3, HK)

            @pl.when((h >= 2) & (i == 2))
            def _():
                serve(2, h - 2, 0)
            return inner

        return lax.fori_loop(0, 3, near_unit, carry)

    lax.fori_loop(0, HK, near_step, 0)

    def far_step(h, carry):
        @pl.when(h < 2)
        def _():
            serve(2, h + 2, 0)

        pair(2, h)
        for g in range(GROUP):
            n = h * GROUP + g
            o = (acc[n] / total[n]).T
            out_ref[0, :, pl.ds(pl.multiple_of(n * HD, HD), HD)] = o.astype(jnp.bfloat16)
        return carry

    lax.fori_loop(0, HK, far_step, 0)

    for j in range(1, NBACK + 1):
        @pl.when(d + j < 16)
        def _():
            seg_copy(j).wait_send()

    def drain(t, carry):
        h = lax.rem(t, HK)
        for step in (1, 3):
            @pl.when((col == 1) | (y + step < 4))
            def _():
                y_copy(0, step, t).wait_send()

        @pl.when(col == 0)
        def _():
            x_copy(t).wait_send()

        @pl.when((h < 2) & (y < 3) & (chip >= 1))
        def _():
            relay_up(t).wait_send()

        @pl.when((h >= 2) & (y == 3))
        def _():
            relay_down(t).wait_send()

        @pl.when((h >= 2) & (y == 1))
        def _():
            direct_far(t).wait_send()

        @pl.when((col == 0) & (y == jnp.where(h < 2, 2, 3)))
        def _():
            park(t).wait_send()

        @pl.when((col == 0) & (y == jnp.where(h < 2, 0, 1)))
        def _():
            cross_spare(t).wait_send()

        @pl.when((h >= 2) & (y == 3))
        def _():
            cross_park(t).wait_send()

        @pl.when(core == 0)
        def _():
            d_copy_own(t).wait_send()

        for k in (1, 2, 3):
            @pl.when(chip >= k)
            def _():
                d_copy(k, t).wait_send()

        @pl.when((col == 1) & (core == 1))
        def _():
            d_copy(4, t).wait_send()
        return carry

    lax.fori_loop(0, 2 * HK, drain, 0)


def body(queries, keys, values, segments):
    hbm = pl.BlockSpec(memory_space=pl.ANY)
    return pl.pallas_call(
        kernel,
        out_shape=jax.ShapeDtypeStruct((1, ROWS, HQ * HD), jnp.bfloat16),
        in_specs=[hbm] * 4,
        out_specs=pl.BlockSpec(memory_space=pltpu.VMEM),
        scratch_shapes=[
            pltpu.VMEM((ROWS, HQ * HD), jnp.bfloat16),
            pltpu.VMEM((ROWS, HK * HD), jnp.bfloat16),
            pltpu.VMEM((NBACK + 2, 2 * HK, ROWS, HD), jnp.bfloat16),
            pltpu.VMEM((NBACK + 1, 1, ROWS), jnp.int32),
            pltpu.VMEM((HQ, HD, ROWS), jnp.bfloat16),
            pltpu.VMEM((NBACK + 1, ROWS, HD), jnp.bfloat16),
            pltpu.VMEM((HD, ROWS), jnp.bfloat16),
            pltpu.VMEM((HALF, ROWS), jnp.float32),
            pltpu.VMEM((HALF, ROWS), jnp.float32),
            pltpu.VMEM((HQ, HD, ROWS), jnp.float32),
            pltpu.VMEM((HQ, 1, ROWS), jnp.float32),
            pltpu.VMEM((HQ, 1, ROWS), jnp.float32),
            pltpu.VMEM((2 * ROWS, ROWS), jnp.float32),
            pltpu.VMEM((2 * ROWS, ROWS), jnp.float32),
            pltpu.VMEM((2 * ROWS, ROWS), jnp.bfloat16),
            pltpu.VMEM((2 * ROWS, ROWS), jnp.bfloat16),
            pltpu.SemaphoreType.DMA((7,)),
            pltpu.SemaphoreType.DMA((NBACK + 2, 2 * HK)),
            pltpu.SemaphoreType.DMA((NBACK + 1,)),
            pltpu.SemaphoreType.DMA((NBACK + 1,)),
            pltpu.SemaphoreType.DMA((2, 2 * HK)),
            pltpu.SemaphoreType.DMA((2 * HK,)),
            pltpu.SemaphoreType.DMA((5, 2 * HK)),
            pltpu.SemaphoreType.DMA((2 * HK,)),
            pltpu.SemaphoreType.DMA((2 * HK,)),
            pltpu.SemaphoreType.DMA((2 * HK,)),
        ],
        compiler_params=pltpu.CompilerParams(collective_id=0, has_side_effects=True),
    )(queries, keys, values, segments)


def solution(mesh):
    placed = (P("dp", "ctx", None), P("dp", "ctx", None), P("dp", "ctx", None), P("dp", "ctx"))
    return jax.shard_map(
        body, mesh=mesh, in_specs=placed, out_specs=P("dp", "ctx", None), check_vma=False
    )
```

```python
import jax
import jax.numpy as jnp
from jax import lax
from jax.experimental import pallas as pl
from jax.experimental.pallas import tpu as pltpu
from jax.sharding import PartitionSpec as P

HQ = 16
HK = 4
HD = 128
GROUP = HQ // HK
HALF = HD // 2
ROWS = 256
NBACK = 8
SPARE = 9
VLIM = 24 << 20
THETA = 500000.0
DEAD = 1048576.0
MESH = pl.DeviceIdType.MESH


def cos_sin(angle):
    n = jnp.floor(angle * 0.6366197723675814 + 0.5)
    r = angle - n * 1.5703125
    r = r - n * 4.837512969970703125e-4
    r = r - n * 7.54978995489188216e-8
    z = r * r
    s = r + r * z * ((-1.9515295891e-4 * z + 8.3321608736e-3) * z - 1.6666654611e-1)
    c = 1.0 - 0.5 * z + z * z * (
        (2.443315711809948e-5 * z - 1.388731625493765e-3) * z + 4.166664568298827e-2
    )
    quarter = n.astype(jnp.int32) & 3
    odd = (quarter & 1) == 1
    cos_mag = jnp.where(odd, s, c)
    sin_mag = jnp.where(odd, c, s)
    cos = jnp.where((quarter == 1) | (quarter == 2), -cos_mag, cos_mag)
    sin = jnp.where(quarter >= 2, -sin_mag, sin_mag)
    return cos, sin


def rotated(block_t, cos, sin):
    wide = block_t.astype(jnp.float32)
    first, second = wide[:HALF], wide[HALF:]
    return jnp.concatenate(
        [first * cos - second * sin, second * cos + first * sin], axis=0
    ).astype(jnp.bfloat16)


def kernel(
    q_hbm, k_hbm, v_hbm, seg_hbm, acc, total,
    q_raw, k_raw, k_t, buf, segs, q_t, m_buf, e_buf, cos_buf, sin_buf, top, s_even, s_odd, p_even, p_odd,
    in_sem, recv_sem, seg_recv, seg_send, y_send, x_send, d_send,
    r_send, f_send, s_send,
):
    d = lax.axis_index("ctx")
    core = lax.rem(d, 2)
    chip = lax.div(d, 2)
    col = lax.div(chip, 4)
    y = lax.rem(chip, 4)
    sibling = d + 1 - 2 * core
    s_buf, p_buf = (s_even, s_odd), (p_even, p_odd)
    scale = float(HD) ** -0.5 * 1.4426950408889634

    own = [
        pltpu.make_async_copy(seg_hbm, segs.at[0], in_sem.at[0]),
        pltpu.make_async_copy(k_hbm.at[0], k_raw, in_sem.at[1]),
        pltpu.make_async_copy(q_hbm.at[0], q_raw, in_sem.at[2]),
    ] + [
        pltpu.make_async_copy(
            v_hbm.at[0, :, pl.ds(h * HD, HD)], buf.at[0, HK + h], in_sem.at[3 + h]
        )
        for h in range(HK)
    ]
    for copy in own:
        copy.start()
    for j in range(1, NBACK + 1):
        segs[j] = jnp.full((1, ROWS), -1, jnp.int32)

    barrier = pltpu.get_barrier_semaphore()
    for k in range(1, 16):
        pl.semaphore_signal(
            barrier, inc=1, device_id={"ctx": lax.rem(d + k, 16)}, device_id_type=MESH
        )
    own[0].wait()
    for h in range(HK):
        own[3 + h].wait()
    pl.semaphore_wait(barrier, 15)

    def copy_to(src_slot, dst_slot, target, sem, t):
        return pltpu.make_async_remote_copy(
            buf.at[src_slot, t], buf.at[dst_slot, t], sem, recv_sem.at[dst_slot, t],
            device_id={"ctx": target}, device_id_type=MESH,
        )

    def ring(step):
        return col * 8 + lax.rem(y + step, 4) * 2 + core

    across = lax.rem(d + 8, 16)

    def y_copy(src_slot, step, t):
        return copy_to(src_slot, 2 * step, ring(step), y_send.at[step // 2, t], t)

    def x_copy(t):
        return copy_to(0, 8, across, x_send.at[t], t)

    def relay_up(t):
        return copy_to(2, 4, ring(1), r_send.at[t], t)

    def relay_down(t):
        return copy_to(6, 4, ring(3), r_send.at[t], t)

    def direct_far(t):
        return copy_to(0, 4, ring(2), f_send.at[t], t)

    def park(t):
        return copy_to(0, SPARE, ring(2), f_send.at[t], t)

    def cross_spare(t):
        return copy_to(SPARE, 4, across, s_send.at[t], t)

    def cross_park(t):
        return copy_to(2, SPARE, across, s_send.at[t], t)

    def wrap_spare(t):
        return copy_to(SPARE, 4, ring(1), s_send.at[t], t)

    def d_copy(k, t):
        return copy_to(2 * k, 2 * k + 1 - 2 * core, sibling, d_send.at[k, t], t)

    def d_copy_own(t):
        return copy_to(0, 1, sibling, d_send.at[0, t], t)

    def seg_copy(j):
        return pltpu.make_async_remote_copy(
            segs.at[0], segs.at[j], seg_send.at[j], seg_recv.at[j],
            device_id={"ctx": lax.rem(d + j, 16)}, device_id_type=MESH,
        )

    def send_own(t):
        for step in (1, 3):
            @pl.when(y + step < 4)
            def _():
                y_copy(0, step, t).start()

        @pl.when(col == 0)
        def _():
            x_copy(t).start()

        @pl.when(core == 0)
        def _():
            d_copy_own(t).start()

    def send_parked(kind):
        for h in range(HK):
            @pl.when((col == 0) & (y == (2 if h < 2 else 3)))
            def _():
                park(kind + h).start()

    def send_direct(kind):
        @pl.when(y == 1)
        def _():
            for h in (2, 3):
                direct_far(kind + h).start()

    for j in range(1, NBACK + 1):
        @pl.when(d + j < 16)
        def _():
            seg_copy(j).start()

    for h in range(HK):
        send_own(HK + h)
    send_parked(HK)

    own[1].wait()
    for h in range(HK):
        k_t[h] = k_raw[:, h * HD : (h + 1) * HD].T
    own[2].wait()

    def turn(n, carry):
        q_t[n] = q_raw[:, pl.ds(pl.multiple_of(n * HD, HD), HD)].T
        return carry

    lax.fori_loop(0, HQ, turn, 0, unroll=4)
    doc = lax.broadcasted_iota(jnp.int32, (HD, ROWS), 0)
    e_buf[...] = jnp.where(doc == segs[0], 1.0, 0.0).astype(jnp.bfloat16)

    for j in range(1, NBACK + 1):
        @pl.when(d >= j)
        def _():
            seg_copy(j).wait_recv()
    seg = segs[0]
    lane = lax.broadcasted_iota(jnp.int32, (1, ROWS), 1).astype(jnp.float32)
    first = jnp.min(seg.astype(jnp.float32), axis=1, keepdims=True)
    seg_f = seg.astype(jnp.float32)
    same = jnp.zeros((1, ROWS), jnp.float32)
    for j in range(1, NBACK + 1):
        same += jnp.where(segs[j].astype(jnp.float32) == first, 1.0, 0.0)
    carried = jnp.sum(same, axis=1, keepdims=True)
    start = jnp.zeros((1, ROWS), jnp.float32)
    for s in range(1, 8):
        before = jnp.sum(jnp.where(seg_f < float(s), 1.0, 0.0), axis=1, keepdims=True)
        start += jnp.where(seg_f == float(s), before, 0.0)
    pos = lane - start + jnp.where(seg_f == first, carried, 0.0)

    freq_index = lax.broadcasted_iota(jnp.int32, (HALF, ROWS), 0).astype(jnp.float32)
    inv_freq = jnp.exp(-jnp.log(jnp.float32(THETA)) * 2.0 * freq_index / HD)
    cos, sin = cos_sin(pos * inv_freq)
    cos_buf[...] = cos
    sin_buf[...] = sin

    for h in range(HK):
        buf[0, h] = rotated(k_t[h], cos, sin).T

    def build_mask(j, carry):
        m_t = jnp.where(doc == segs[j], 0.0, -DEAD).astype(jnp.bfloat16)
        m_buf[j] = m_t.T
        return carry

    lax.fori_loop(0, 2, build_mask, 0)
    for h in range(HK):
        send_own(h)
    send_parked(0)
    lax.fori_loop(2, NBACK + 1, build_mask, 0, unroll=7)

    def wait_in(slot, t):
        pltpu.make_async_remote_copy(
            buf.at[slot, t], buf.at[slot, t], d_send.at[0, t], recv_sem.at[slot, t],
            device_id={"ctx": sibling}, device_id_type=MESH,
        ).wait_recv()

    def serve(k, h, kind):
        t = h + kind

        @pl.when(chip >= k)
        def _():
            wait_in(2 * k, t)
            if k == 4:
                for step in (1, 3):
                    @pl.when(y + step >= 4)
                    def _():
                        y_copy(8, step, t).start()

                @pl.when(core == 1)
                def _():
                    d_copy(k, t).start()
                return
            if k == 1:
                @pl.when((h >= 2) & (col == 0) & (y == 3))
                def _():
                    cross_park(t).start()
            d_copy(k, t).start()

    def relay():
        for h in range(HK):
            for t in (HK + h, h):
                if h < 2:
                    @pl.when((chip >= 1) & (y < 3))
                    def _():
                        relay_up(t).start()
                else:
                    @pl.when(y == 3)
                    def _():
                        relay_down(t).start()

    def serve_spare(h, kind):
        t = h + kind

        @pl.when((col == 0) & (y == jnp.where(h < 2, 0, 1)))
        def _():
            wait_in(SPARE, t)
            cross_spare(t).start()

        @pl.when((col == 1) & (y == 3) & (h >= 2))
        def _():
            wait_in(SPARE, t)
            wrap_spare(t).start()

    def pipeline(stages, ahead=None):
        def scores(i):
            slots, h, g, is_own = stages[i]
            n = h * GROUP + g
            quer = jnp.concatenate([q_t[n], e_buf[...]], axis=0)
            peak = None if is_own else top[n]
            for a, slot in enumerate(slots):
                keys = jnp.concatenate([buf[slot, h], m_buf[slot]], axis=1)
                s = jnp.dot(keys, quer, preferred_element_type=jnp.float32)
                if is_own and a == 0:
                    later = lax.broadcasted_iota(jnp.int32, (ROWS, ROWS), 0) > (
                        lax.broadcasted_iota(jnp.int32, (ROWS, ROWS), 1)
                    )
                    s = jnp.where(later, -DEAD, s)
                s_buf[i % 2][pl.ds(a * ROWS, ROWS)] = s
                high = jnp.max(s, axis=0, keepdims=True)
                peak = high if peak is None else jnp.maximum(peak, high)
            return peak

        def weigh(i, peak):
            slots, h, g, is_own = stages[i]
            n = h * GROUP + g
            fade = None if is_own else jnp.exp2((top[n] - peak) * scale)
            top[n] = peak
            for a in range(len(slots)):
                p = jnp.exp2((s_buf[i % 2][pl.ds(a * ROWS, ROWS)] - peak) * scale)
                p_buf[i % 2][pl.ds(a * ROWS, ROWS)] = p.astype(jnp.bfloat16)
            return fade

        def add_up(i, fade):
            slots, h, g, is_own = stages[i]
            n = h * GROUP + g
            width = len(slots) * ROWS
            vals = jnp.concatenate([buf[slot, HK + h].T for slot in slots], axis=1)
            vals = jnp.concatenate([vals, jnp.ones((16, width), jnp.bfloat16)], axis=0)
            o = jnp.dot(vals, p_buf[i % 2][pl.ds(0, width)], preferred_element_type=jnp.float32)
            if is_own:
                acc[n] = o[:HD]
                total[n] = o[HD : HD + 1]
            else:
                acc[n] = acc[n] * fade + o[:HD]
                total[n] = total[n] * fade + o[HD : HD + 1]

        peaks, fades = {}, {}
        for i in range(len(stages) + 2):
            if ahead is not None and i < len(stages) and i % GROUP == 0:
                ahead(i // GROUP)
            if i < len(stages):
                peaks[i] = scores(i)
            if i >= 2:
                add_up(i - 2, fades[i - 2])
            if 1 <= i <= len(stages):
                fades[i - 1] = weigh(i - 1, peaks[i - 1])

    def heads(slots, h, is_own=False):
        return [(slots, h, g, is_own) for g in range(GROUP)]

    def wait_both(slot, h):
        wait_in(slot, HK + h)
        wait_in(slot, h)

    def spin(h):
        for g in range(GROUP):
            n = h * GROUP + g
            q_t[n] = rotated(q_t[n], cos_buf[...], sin_buf[...])

    def own_step(i, carry):
        h = 2 * i

        def ahead(part):
            if part == 1:
                serve(4, h + 1, HK)

        serve(4, h, HK)

        @pl.when(i == 1)
        def _():
            serve(1, 1, HK)
            serve(3, 1, HK)

        spin(h)
        spin(h + 1)

        @pl.when(core == 0)
        def _():
            pipeline(heads([0], h, True) + heads([0], h + 1, True), ahead)

        @pl.when(core == 1)
        def _():
            wait_both(1, h)
            wait_both(1, h + 1)
            pipeline(heads([0, 1], h, True) + heads([0, 1], h + 1, True), ahead)

        serve(1, h, HK)
        serve(3, h, HK)
        return carry

    lax.fori_loop(0, HK // 2, own_step, 0)
    send_direct(HK)
    serve(1, 3, HK)
    serve(3, 3, HK)
    serve(4, 0, 0)
    serve(4, 1, 0)

    def cross_step(i, carry):
        h = 2 * i

        def ahead_of(slot):
            def ahead(part):
                if slot is not None:
                    wait_both(slot, h + part)
                if part == 1:
                    @pl.when(i == 0)
                    def _():
                        serve(4, 2, 0)
                        serve(1, 0, 0)
                        serve(3, 0, 0)
            return ahead

        @pl.when((col == 1) & (core == 0))
        def _():
            pipeline(heads([8, 7], h) + heads([8, 7], h + 1), ahead_of(7))

        @pl.when((col == 1) & (core == 1))
        def _():
            pipeline(heads([8], h) + heads([8], h + 1), ahead_of(None))

        @pl.when((col == 0) & (i == 0))
        def _():
            serve(1, 0, 0)
            serve(3, 0, 0)

        @pl.when(i == 0)
        def _():
            serve(4, 3, 0)
            send_direct(0)
            serve(1, 1, 0)
            serve(3, 1, 0)

        return carry

    lax.fori_loop(0, HK // 2, cross_step, 0)
    serve(1, 2, 0)
    serve(3, 2, 0)

    def near_step(h, carry):
        def between(part):
            @pl.when((h == 0) & (part == 1))
            def _():
                serve(1, 3, 0)
                serve(3, 3, 0)
                relay()
                for u in range(HK):
                    serve_spare(u, HK)

            @pl.when((h == 1) & (part == 1))
            def _():
                for u in range(HK):
                    serve_spare(u, 0)

            @pl.when((h == 2) & (part == 1))
            def _():
                serve(2, 0, HK)
                serve(2, 0, 0)

            @pl.when((h == 3) & (part == 1))
            def _():
                serve(2, 1, HK)
                serve(2, 1, 0)

        slots = [2 * k - 1 + 2 * core for k in (1, 3)]

        @pl.when(col == 1)
        def _():
            def ahead(part):
                if part == 1:
                    between(1)
                wait_both(slots[part], h)

            pipeline(heads([2, slots[0]], h) + heads([6, slots[1]], h), ahead)

        @pl.when(col == 0)
        def _():
            between(1)

            def small(i, inner):
                k = 2 * i + 1

                @pl.when(chip >= k)
                def _():
                    slot = 2 * k - 1 + 2 * core
                    wait_both(slot, h)
                    pipeline(heads([2 * k, slot], h))
                return inner

            lax.fori_loop(0, 2, small, 0)

        return carry

    lax.fori_loop(0, HK, near_step, 0)

    def far_step(i, carry):
        h = 2 * i

        @pl.when(i == 1)
        def _():
            serve(2, 2, HK)
            serve(2, 3, HK)
            serve(2, 2, 0)
            serve(2, 3, 0)

        @pl.when(chip >= 2)
        def _():
            slot = 3 + 2 * core

            def ahead(part):
                wait_both(slot, h + part)

            pipeline(heads([4, slot], h) + heads([4, slot], h + 1), ahead)
        return carry

    lax.fori_loop(0, HK // 2, far_step, 0)

    for j in range(1, NBACK + 1):
        @pl.when(d + j < 16)
        def _():
            seg_copy(j).wait_send()

    def drain(t, carry):
        h = lax.rem(t, HK)
        for step in (1, 3):
            @pl.when((col == 1) | (y + step < 4))
            def _():
                y_copy(0, step, t).wait_send()

        @pl.when(col == 0)
        def _():
            x_copy(t).wait_send()

        @pl.when((h < 2) & (y < 3) & (chip >= 1))
        def _():
            relay_up(t).wait_send()

        @pl.when((h >= 2) & (y == 3))
        def _():
            relay_down(t).wait_send()

        @pl.when((h >= 2) & (y == 1))
        def _():
            direct_far(t).wait_send()

        @pl.when((col == 0) & (y == jnp.where(h < 2, 2, 3)))
        def _():
            park(t).wait_send()

        @pl.when((col == 0) & (y == jnp.where(h < 2, 0, 1)))
        def _():
            cross_spare(t).wait_send()

        @pl.when((h >= 2) & (y == 3))
        def _():
            cross_park(t).wait_send()

        @pl.when(core == 0)
        def _():
            d_copy_own(t).wait_send()

        for k in (1, 2, 3):
            @pl.when(chip >= k)
            def _():
                d_copy(k, t).wait_send()

        @pl.when((col == 1) & (core == 1))
        def _():
            d_copy(4, t).wait_send()
        return carry

    lax.fori_loop(0, 2 * HK, drain, 0)


def finish(acc, total, out):
    for g in range(GROUP):
        o = (acc[g] / total[g]).T
        out[0, :, g * HD : (g + 1) * HD] = o.astype(jnp.bfloat16)


def body(queries, keys, values, segments):
    hbm = pl.BlockSpec(memory_space=pltpu.HBM)
    acc, total = pl.pallas_call(
        kernel,
        out_shape=(
            jax.ShapeDtypeStruct((HQ, HD, ROWS), jnp.float32),
            jax.ShapeDtypeStruct((HQ, 1, ROWS), jnp.float32),
        ),
        in_specs=[hbm] * 4,
        out_specs=(pl.BlockSpec(memory_space=pltpu.VMEM),) * 2,
        scratch_shapes=[
            pltpu.VMEM((ROWS, HQ * HD), jnp.bfloat16),
            pltpu.VMEM((ROWS, HK * HD), jnp.bfloat16),
            pltpu.VMEM((HK, HD, ROWS), jnp.bfloat16),
            pltpu.VMEM((NBACK + 2, 2 * HK, ROWS, HD), jnp.bfloat16),
            pltpu.VMEM((NBACK + 1, 1, ROWS), jnp.int32),
            pltpu.VMEM((HQ, HD, ROWS), jnp.bfloat16),
            pltpu.VMEM((NBACK + 1, ROWS, HD), jnp.bfloat16),
            pltpu.VMEM((HD, ROWS), jnp.bfloat16),
            pltpu.VMEM((HALF, ROWS), jnp.float32),
            pltpu.VMEM((HALF, ROWS), jnp.float32),
            pltpu.VMEM((HQ, 1, ROWS), jnp.float32),
            pltpu.VMEM((2 * ROWS, ROWS), jnp.float32),
            pltpu.VMEM((2 * ROWS, ROWS), jnp.float32),
            pltpu.VMEM((2 * ROWS, ROWS), jnp.bfloat16),
            pltpu.VMEM((2 * ROWS, ROWS), jnp.bfloat16),
            pltpu.SemaphoreType.DMA((7,)),
            pltpu.SemaphoreType.DMA((NBACK + 2, 2 * HK)),
            pltpu.SemaphoreType.DMA((NBACK + 1,)),
            pltpu.SemaphoreType.DMA((NBACK + 1,)),
            pltpu.SemaphoreType.DMA((2, 2 * HK)),
            pltpu.SemaphoreType.DMA((2 * HK,)),
            pltpu.SemaphoreType.DMA((5, 2 * HK)),
            pltpu.SemaphoreType.DMA((2 * HK,)),
            pltpu.SemaphoreType.DMA((2 * HK,)),
            pltpu.SemaphoreType.DMA((2 * HK,)),
        ],
        compiler_params=pltpu.CompilerParams(collective_id=0, has_side_effects=True, vmem_limit_bytes=VLIM),
    )(*(pltpu.with_memory_space_constraint(x, pltpu.HBM) for x in (queries, keys, values, segments)))
    return pl.pallas_call(
        finish,
        grid=(HK,),
        out_shape=jax.ShapeDtypeStruct((1, ROWS, HQ * HD), jnp.bfloat16),
        in_specs=[
            pl.BlockSpec((GROUP, HD, ROWS), lambda h: (h, 0, 0)),
            pl.BlockSpec((GROUP, 1, ROWS), lambda h: (h, 0, 0)),
        ],
        out_specs=pl.BlockSpec((1, ROWS, GROUP * HD), lambda h: (0, 0, h)),
        compiler_params=pltpu.CompilerParams(vmem_limit_bytes=8 << 20),
    )(acc, total)


def solution(mesh):
    placed = (P("dp", "ctx", None), P("dp", "ctx", None), P("dp", "ctx", None), P("dp", "ctx"))
    return jax.shard_map(
        body, mesh=mesh, in_specs=placed, out_specs=P("dp", "ctx", None), check_vma=False
    )
```

```python
import jax
import jax.numpy as jnp
from jax import lax
from jax.experimental import pallas as pl
from jax.experimental.pallas import tpu as pltpu
from jax.sharding import PartitionSpec as P

HQ = 16
HK = 4
HD = 128
GROUP = HQ // HK
HALF = HD // 2
ROWS = 256
NBACK = 8
SPARE = 9
VLIM = 24 << 20
THETA = 500000.0
DEAD = 1048576.0
MESH = pl.DeviceIdType.MESH


def cos_sin(angle):
    n = jnp.floor(angle * 0.6366197723675814 + 0.5)
    r = angle - n * 1.5703125
    r = r - n * 4.837512969970703125e-4
    r = r - n * 7.54978995489188216e-8
    z = r * r
    s = r + r * z * ((-1.9515295891e-4 * z + 8.3321608736e-3) * z - 1.6666654611e-1)
    c = 1.0 - 0.5 * z + z * z * (
        (2.443315711809948e-5 * z - 1.388731625493765e-3) * z + 4.166664568298827e-2
    )
    quarter = n.astype(jnp.int32) & 3
    odd = (quarter & 1) == 1
    cos_mag = jnp.where(odd, s, c)
    sin_mag = jnp.where(odd, c, s)
    cos = jnp.where((quarter == 1) | (quarter == 2), -cos_mag, cos_mag)
    sin = jnp.where(quarter >= 2, -sin_mag, sin_mag)
    return cos, sin


def rotated(block_t, cos, sin):
    wide = block_t.astype(jnp.float32)
    first, second = wide[:HALF], wide[HALF:]
    return jnp.concatenate(
        [first * cos - second * sin, second * cos + first * sin], axis=0
    ).astype(jnp.bfloat16)


def kernel(
    q_hbm, k_hbm, v_hbm, seg_hbm, acc, total,
    q_raw, k_raw, k_t, buf, segs, q_t, m_buf, e_buf, cos_buf, sin_buf, top, s_even, s_odd, p_even, p_odd,
    in_sem, recv_sem, seg_recv, seg_send, y_send, x_send, d_send,
    r_send, f_send, s_send,
):
    d = lax.axis_index("ctx")
    core = lax.rem(d, 2)
    chip = lax.div(d, 2)
    col = lax.div(chip, 4)
    y = lax.rem(chip, 4)
    sibling = d + 1 - 2 * core
    s_buf, p_buf = (s_even, s_odd), (p_even, p_odd)
    scale = float(HD) ** -0.5 * 1.4426950408889634

    own = [
        pltpu.make_async_copy(seg_hbm, segs.at[0], in_sem.at[0]),
        pltpu.make_async_copy(k_hbm.at[0], k_raw, in_sem.at[1]),
        pltpu.make_async_copy(q_hbm.at[0], q_raw, in_sem.at[2]),
    ] + [
        pltpu.make_async_copy(
            v_hbm.at[0, :, pl.ds(h * HD, HD)], buf.at[0, HK + h], in_sem.at[3 + h]
        )
        for h in range(HK)
    ]
    for copy in own:
        copy.start()
    for j in range(1, NBACK + 1):
        segs[j] = jnp.full((1, ROWS), -1, jnp.int32)

    barrier = pltpu.get_barrier_semaphore()
    for k in range(1, 16):
        pl.semaphore_signal(
            barrier, inc=1, device_id={"ctx": lax.rem(d + k, 16)}, device_id_type=MESH
        )
    own[0].wait()
    for h in range(HK):
        own[3 + h].wait()
    pl.semaphore_wait(barrier, 15)

    def copy_to(src_slot, dst_slot, target, sem, t):
        return pltpu.make_async_remote_copy(
            buf.at[src_slot, t], buf.at[dst_slot, t], sem, recv_sem.at[dst_slot, t],
            device_id={"ctx": target}, device_id_type=MESH,
        )

    def ring(step):
        return col * 8 + lax.rem(y + step, 4) * 2 + core

    across = lax.rem(d + 8, 16)

    def y_copy(src_slot, step, t):
        return copy_to(src_slot, 2 * step, ring(step), y_send.at[step // 2], t)

    def x_copy(t):
        return copy_to(0, 8, across, x_send.at[0], t)

    def relay_up(t):
        return copy_to(2, 4, ring(1), r_send.at[0], t)

    def relay_down(t):
        return copy_to(6, 4, ring(3), r_send.at[0], t)

    def direct_far(t):
        return copy_to(0, 4, ring(2), f_send.at[0], t)

    def park(t):
        return copy_to(0, SPARE, ring(2), f_send.at[0], t)

    def cross_spare(t):
        return copy_to(SPARE, 4, across, s_send.at[0], t)

    def cross_park(t):
        return copy_to(2, SPARE, across, s_send.at[0], t)

    def wrap_spare(t):
        return copy_to(SPARE, 4, ring(1), s_send.at[0], t)

    def d_copy(k, t):
        return copy_to(2 * k, 2 * k + 1 - 2 * core, sibling, d_send.at[k], t)

    def d_copy_own(t):
        return copy_to(0, 1, sibling, d_send.at[0], t)

    def seg_copy(j):
        return pltpu.make_async_remote_copy(
            segs.at[0], segs.at[j], seg_send.at[j], seg_recv.at[j],
            device_id={"ctx": lax.rem(d + j, 16)}, device_id_type=MESH,
        )

    def send_own(t):
        for step in (1, 3):
            @pl.when(y + step < 4)
            def _():
                y_copy(0, step, t).start()

        @pl.when(col == 0)
        def _():
            x_copy(t).start()

        @pl.when(core == 0)
        def _():
            d_copy_own(t).start()

    def send_parked(kind):
        for h in range(HK):
            @pl.when((col == 0) & (y == (2 if h < 2 else 3)))
            def _():
                park(kind + h).start()

    def send_direct(where):
        @pl.when((y == 1) & (col == where))
        def _():
            for h in (2, 3):
                direct_far(HK + h).start()
                direct_far(h).start()

    for j in range(1, NBACK + 1):
        @pl.when(d + j < 16)
        def _():
            seg_copy(j).start()

    for h in range(HK):
        send_own(HK + h)
    send_parked(HK)

    own[1].wait()
    for h in range(HK):
        k_t[h] = k_raw[:, h * HD : (h + 1) * HD].T
    own[2].wait()

    def turn(n, carry):
        q_t[n] = q_raw[:, pl.ds(pl.multiple_of(n * HD, HD), HD)].T
        return carry

    lax.fori_loop(0, HQ, turn, 0, unroll=4)
    doc = lax.broadcasted_iota(jnp.int32, (HD, ROWS), 0)
    e_buf[...] = jnp.where(doc == segs[0], 1.0, 0.0).astype(jnp.bfloat16)

    for j in range(1, NBACK + 1):
        @pl.when(d >= j)
        def _():
            seg_copy(j).wait_recv()
    seg = segs[0]
    lane = lax.broadcasted_iota(jnp.int32, (1, ROWS), 1).astype(jnp.float32)
    first = jnp.min(seg.astype(jnp.float32), axis=1, keepdims=True)
    seg_f = seg.astype(jnp.float32)
    same = jnp.zeros((1, ROWS), jnp.float32)
    for j in range(1, NBACK + 1):
        same += jnp.where(segs[j].astype(jnp.float32) == first, 1.0, 0.0)
    carried = jnp.sum(same, axis=1, keepdims=True)
    start = jnp.zeros((1, ROWS), jnp.float32)
    for s in range(1, 8):
        before = jnp.sum(jnp.where(seg_f < float(s), 1.0, 0.0), axis=1, keepdims=True)
        start += jnp.where(seg_f == float(s), before, 0.0)
    pos = lane - start + jnp.where(seg_f == first, carried, 0.0)

    freq_index = lax.broadcasted_iota(jnp.int32, (HALF, ROWS), 0).astype(jnp.float32)
    inv_freq = jnp.exp(-jnp.log(jnp.float32(THETA)) * 2.0 * freq_index / HD)
    cos, sin = cos_sin(pos * inv_freq)
    cos_buf[...] = cos
    sin_buf[...] = sin

    for h in range(HK):
        buf[0, h] = rotated(k_t[h], cos, sin).T

    def build_mask(j, carry):
        m_t = jnp.where(doc == segs[j], 0.0, -DEAD).astype(jnp.bfloat16)
        m_buf[j] = m_t.T
        return carry

    lax.fori_loop(0, 2, build_mask, 0)
    for h in range(HK):
        send_own(h)
    send_parked(0)
    lax.fori_loop(2, NBACK + 1, build_mask, 0, unroll=7)

    def wait_in(slot, t):
        pltpu.make_async_remote_copy(
            buf.at[slot, t], buf.at[slot, t], d_send.at[0], recv_sem.at[slot, t],
            device_id={"ctx": sibling}, device_id_type=MESH,
        ).wait_recv()

    def serve(k, h, kind):
        t = h + kind

        @pl.when(chip >= k)
        def _():
            wait_in(2 * k, t)
            if k == 4:
                for step in (1, 3):
                    @pl.when(y + step >= 4)
                    def _():
                        y_copy(8, step, t).start()

                @pl.when(core == 1)
                def _():
                    d_copy(k, t).start()
                return
            if k == 1:
                @pl.when((h >= 2) & (col == 0) & (y == 3))
                def _():
                    cross_park(t).start()
            d_copy(k, t).start()

    def relay():
        for h in range(HK):
            for t in (HK + h, h):
                if h < 2:
                    @pl.when((chip >= 1) & (y < 3))
                    def _():
                        relay_up(t).start()
                else:
                    @pl.when(y == 3)
                    def _():
                        relay_down(t).start()

    def serve_spare(h, kind):
        t = h + kind

        @pl.when((col == 0) & (y == jnp.where(h < 2, 0, 1)))
        def _():
            wait_in(SPARE, t)
            cross_spare(t).start()

        @pl.when((col == 1) & (y == 3) & (h >= 2))
        def _():
            wait_in(SPARE, t)
            wrap_spare(t).start()

    def pipeline(stages, ahead=None):
        def scores(i):
            slots, h, g, is_own = stages[i]
            n = h * GROUP + g
            quer = jnp.concatenate([q_t[n], e_buf[...]], axis=0)
            peak = None if is_own else top[n]
            for a, slot in enumerate(slots):
                keys = jnp.concatenate([buf[slot, h], m_buf[slot]], axis=1)
                s = jnp.dot(keys, quer, preferred_element_type=jnp.float32)
                if is_own and a == 0:
                    later = lax.broadcasted_iota(jnp.int32, (ROWS, ROWS), 0) > (
                        lax.broadcasted_iota(jnp.int32, (ROWS, ROWS), 1)
                    )
                    s = jnp.where(later, -DEAD, s)
                s_buf[i % 2][pl.ds(a * ROWS, ROWS)] = s
                high = jnp.max(s, axis=0, keepdims=True)
                peak = high if peak is None else jnp.maximum(peak, high)
            return peak

        def weigh(i, peak):
            slots, h, g, is_own = stages[i]
            n = h * GROUP + g
            fade = None if is_own else jnp.exp2((top[n] - peak) * scale)
            top[n] = peak
            for a in range(len(slots)):
                p = jnp.exp2((s_buf[i % 2][pl.ds(a * ROWS, ROWS)] - peak) * scale)
                p_buf[i % 2][pl.ds(a * ROWS, ROWS)] = p.astype(jnp.bfloat16)
            return fade

        def add_up(i, fade):
            slots, h, g, is_own = stages[i]
            n = h * GROUP + g
            width = len(slots) * ROWS
            vals = jnp.concatenate([buf[slot, HK + h].T for slot in slots], axis=1)
            vals = jnp.concatenate([vals, jnp.ones((16, width), jnp.bfloat16)], axis=0)
            o = jnp.dot(vals, p_buf[i % 2][pl.ds(0, width)], preferred_element_type=jnp.float32)
            if is_own:
                acc[n] = o[:HD]
                total[n] = o[HD : HD + 1]
            else:
                acc[n] = acc[n] * fade + o[:HD]
                total[n] = total[n] * fade + o[HD : HD + 1]

        peaks, fades = {}, {}
        for i in range(len(stages) + 2):
            if ahead is not None and i < len(stages) and i % GROUP == 0:
                ahead(i // GROUP)
            if i < len(stages):
                peaks[i] = scores(i)
            if i >= 2:
                add_up(i - 2, fades[i - 2])
            if 1 <= i <= len(stages):
                fades[i - 1] = weigh(i - 1, peaks[i - 1])

    def heads(slots, h, is_own=False):
        return [(slots, h, g, is_own) for g in range(GROUP)]

    def wait_both(slot, h):
        wait_in(slot, HK + h)
        wait_in(slot, h)

    def spin(h):
        for g in range(GROUP):
            n = h * GROUP + g
            q_t[n] = rotated(q_t[n], cos_buf[...], sin_buf[...])

    def own_step(i, carry):
        h = 2 * i

        def ahead(part):
            if part == 1:
                serve(4, h + 1, HK)

        serve(4, h, HK)
        spin(h)
        spin(h + 1)

        @pl.when(core == 0)
        def _():
            pipeline(heads([0], h, True) + heads([0], h + 1, True), ahead)

        @pl.when(core == 1)
        def _():
            wait_both(1, h)
            wait_both(1, h + 1)
            pipeline(heads([0, 1], h, True) + heads([0, 1], h + 1, True), ahead)

        return carry

    def serve_sides(h, kind):
        serve(1, h, kind)
        serve(3, h, kind)

    lax.fori_loop(0, HK // 2, own_step, 0)
    serve(4, 0, 0)
    serve_sides(0, HK)
    serve(4, 1, 0)

    def cross_step(i, carry):
        h = 2 * i

        def ahead_of(slot):
            def ahead(part):
                if slot is not None:
                    wait_both(slot, h + part)
                if part == 1:
                    @pl.when(i == 0)
                    def _():
                        serve(4, 2, 0)
                        serve_sides(1, HK)

                    @pl.when(i == 1)
                    def _():
                        serve_sides(0, 0)
            return ahead

        @pl.when((col == 1) & (core == 0))
        def _():
            pipeline(heads([8, 7], h) + heads([8, 7], h + 1), ahead_of(7))

        @pl.when((col == 1) & (core == 1))
        def _():
            pipeline(heads([8], h) + heads([8], h + 1), ahead_of(None))

        @pl.when((col == 0) & (i == 0))
        def _():
            serve_sides(1, HK)

        @pl.when((col == 0) & (i == 1))
        def _():
            serve_sides(0, 0)

        @pl.when(i == 0)
        def _():
            serve(4, 3, 0)
            send_direct(1)
            serve_sides(2, HK)
            serve_sides(3, HK)

        return carry

    lax.fori_loop(0, HK // 2, cross_step, 0)
    serve_sides(1, 0)

    def near_step(h, carry):
        def between(part):
            @pl.when((h == 0) & (part == 1))
            def _():
                serve_sides(2, 0)
                serve_sides(3, 0)
                send_direct(0)
                relay()
                for u in range(HK):
                    serve_spare(u, HK)

            @pl.when((h == 1 + col) & (part == 1))
            def _():
                for u in range(HK):
                    serve_spare(u, 0)

            @pl.when((h == 3) & (part == 1))
            def _():
                for u in (0, 1):
                    serve(2, u, HK)
                    serve(2, u, 0)

        slots = [2 * k - 1 + 2 * core for k in (1, 3)]

        @pl.when(col == 1)
        def _():
            def ahead(part):
                if part == 1:
                    between(1)
                wait_both(slots[part], h)

            pipeline(heads([2, slots[0]], h) + heads([6, slots[1]], h), ahead)

        @pl.when(col == 0)
        def _():
            between(1)

            def small(i, inner):
                k = 2 * i + 1

                @pl.when(chip >= k)
                def _():
                    slot = 2 * k - 1 + 2 * core
                    wait_both(slot, h)
                    pipeline(heads([2 * k, slot], h))
                return inner

            lax.fori_loop(0, 2, small, 0)

        return carry

    lax.fori_loop(0, HK, near_step, 0)

    def far_step(i, carry):
        h = 2 * i

        @pl.when(chip >= 2)
        def _():
            slot = 3 + 2 * core

            def ahead(part):
                if part == 1:
                    @pl.when(i == 0)
                    def _():
                        for u in (2, 3):
                            serve(2, u, HK)
                            serve(2, u, 0)

                wait_both(slot, h + part)

            pipeline(heads([4, slot], h) + heads([4, slot], h + 1), ahead)
        return carry

    lax.fori_loop(0, HK // 2, far_step, 0)

    for j in range(1, NBACK + 1):
        @pl.when(d + j < 16)
        def _():
            seg_copy(j).wait_send()

    def drain(sem, chunks):
        ref = buf.at[0, pl.ds(0, chunks)]
        pltpu.make_async_remote_copy(
            ref, ref, sem, recv_sem.at[0, 0], device_id={"ctx": sibling}, device_id_type=MESH
        ).wait_send()

    for step in (1, 3):
        @pl.when((col == 1) | (y + step < 4))
        def _():
            drain(y_send.at[step // 2], 2 * HK)

    @pl.when(col == 0)
    def _():
        drain(x_send.at[0], 2 * HK)

    @pl.when((chip >= 1) | (y == 3))
    def _():
        drain(r_send.at[0], HK)

    @pl.when((y == 1) | ((col == 0) & (y >= 2)))
    def _():
        drain(f_send.at[0], HK)

    @pl.when((y == 3) | ((col == 0) & (y < 2)))
    def _():
        drain(s_send.at[0], HK)

    @pl.when(core == 0)
    def _():
        drain(d_send.at[0], 2 * HK)

    for k in (1, 2, 3):
        @pl.when(chip >= k)
        def _():
            drain(d_send.at[k], 2 * HK)

    @pl.when((col == 1) & (core == 1))
    def _():
        drain(d_send.at[4], 2 * HK)


def finish(acc, total, out):
    for g in range(GROUP):
        o = (acc[g] / total[g]).astype(jnp.bfloat16)
        out[0, :, g * HD : (g + 1) * HD] = o.T


def body(queries, keys, values, segments):
    hbm = pl.BlockSpec(memory_space=pltpu.HBM)
    acc, total = pl.pallas_call(
        kernel,
        out_shape=(
            jax.ShapeDtypeStruct((HQ, HD, ROWS), jnp.float32),
            jax.ShapeDtypeStruct((HQ, 1, ROWS), jnp.float32),
        ),
        in_specs=[hbm] * 4,
        out_specs=(pl.BlockSpec(memory_space=pltpu.VMEM),) * 2,
        scratch_shapes=[
            pltpu.VMEM((ROWS, HQ * HD), jnp.bfloat16),
            pltpu.VMEM((ROWS, HK * HD), jnp.bfloat16),
            pltpu.VMEM((HK, HD, ROWS), jnp.bfloat16),
            pltpu.VMEM((NBACK + 2, 2 * HK, ROWS, HD), jnp.bfloat16),
            pltpu.VMEM((NBACK + 1, 1, ROWS), jnp.int32),
            pltpu.VMEM((HQ, HD, ROWS), jnp.bfloat16),
            pltpu.VMEM((NBACK + 1, ROWS, HD), jnp.bfloat16),
            pltpu.VMEM((HD, ROWS), jnp.bfloat16),
            pltpu.VMEM((HALF, ROWS), jnp.float32),
            pltpu.VMEM((HALF, ROWS), jnp.float32),
            pltpu.VMEM((HQ, 1, ROWS), jnp.float32),
            pltpu.VMEM((2 * ROWS, ROWS), jnp.float32),
            pltpu.VMEM((2 * ROWS, ROWS), jnp.float32),
            pltpu.VMEM((2 * ROWS, ROWS), jnp.bfloat16),
            pltpu.VMEM((2 * ROWS, ROWS), jnp.bfloat16),
            pltpu.SemaphoreType.DMA((7,)),
            pltpu.SemaphoreType.DMA((NBACK + 2, 2 * HK)),
            pltpu.SemaphoreType.DMA((NBACK + 1,)),
            pltpu.SemaphoreType.DMA((NBACK + 1,)),
            pltpu.SemaphoreType.DMA((2,)),
            pltpu.SemaphoreType.DMA((1,)),
            pltpu.SemaphoreType.DMA((5,)),
            pltpu.SemaphoreType.DMA((1,)),
            pltpu.SemaphoreType.DMA((1,)),
            pltpu.SemaphoreType.DMA((1,)),
        ],
        compiler_params=pltpu.CompilerParams(collective_id=0, has_side_effects=True, vmem_limit_bytes=VLIM),
    )(*(pltpu.with_memory_space_constraint(x, pltpu.HBM) for x in (queries, keys, values, segments)))
    return pl.pallas_call(
        finish,
        grid=(HK,),
        out_shape=jax.ShapeDtypeStruct((1, ROWS, HQ * HD), jnp.bfloat16),
        in_specs=[
            pl.BlockSpec((GROUP, HD, ROWS), lambda h: (h, 0, 0)),
            pl.BlockSpec((GROUP, 1, ROWS), lambda h: (h, 0, 0)),
        ],
        out_specs=pl.BlockSpec((1, ROWS, GROUP * HD), lambda h: (0, 0, h)),
        compiler_params=pltpu.CompilerParams(vmem_limit_bytes=8 << 20),
    )(acc, total)


def solution(mesh):
    placed = (P("dp", "ctx", None), P("dp", "ctx", None), P("dp", "ctx", None), P("dp", "ctx"))
    return jax.shard_map(
        body, mesh=mesh, in_specs=placed, out_specs=P("dp", "ctx", None), check_vma=False
    )
```

```python
import jax
import jax.numpy as jnp
from jax import lax
from jax.experimental import pallas as pl
from jax.experimental.pallas import tpu as pltpu
from jax.sharding import PartitionSpec as P

HQ = 16
HK = 4
HD = 128
GROUP = HQ // HK
HALF = HD // 2
ROWS = 256
NBACK = 8
SPARE = 9
VLIM = 24 << 20
THETA = 500000.0
DEAD = 1048576.0
MESH = pl.DeviceIdType.MESH


def cos_sin(angle):
    n = jnp.floor(angle * 0.6366197723675814 + 0.5)
    r = angle - n * 1.5703125
    r = r - n * 4.837512969970703125e-4
    r = r - n * 7.54978995489188216e-8
    z = r * r
    s = r + r * z * ((-1.9515295891e-4 * z + 8.3321608736e-3) * z - 1.6666654611e-1)
    c = 1.0 - 0.5 * z + z * z * (
        (2.443315711809948e-5 * z - 1.388731625493765e-3) * z + 4.166664568298827e-2
    )
    quarter = n.astype(jnp.int32) & 3
    odd = (quarter & 1) == 1
    cos_mag = jnp.where(odd, s, c)
    sin_mag = jnp.where(odd, c, s)
    cos = jnp.where((quarter == 1) | (quarter == 2), -cos_mag, cos_mag)
    sin = jnp.where(quarter >= 2, -sin_mag, sin_mag)
    return cos, sin


def rotated(block_t, cos, sin):
    wide = block_t.astype(jnp.float32)
    first, second = wide[:HALF], wide[HALF:]
    return jnp.concatenate(
        [first * cos - second * sin, second * cos + first * sin], axis=0
    ).astype(jnp.bfloat16)


def kernel(
    q_hbm, k_hbm, v_hbm, seg_hbm, acc, total,
    q_raw, k_raw, k_t, buf, segs, q_t, m_buf, e_buf, cos_buf, sin_buf, top, s_even, s_odd, p_even, p_odd,
    local_pos, first_doc,
    in_sem, recv_sem, seg_recv, seg_send, y_send, x_send, d_send,
    r_send, f_send, s_send,
):
    d = lax.axis_index("ctx")
    core = lax.rem(d, 2)
    chip = lax.div(d, 2)
    col = lax.div(chip, 4)
    y = lax.rem(chip, 4)
    sibling = d + 1 - 2 * core
    s_buf, p_buf = (s_even, s_odd), (p_even, p_odd)
    scale = float(HD) ** -0.5 * 1.4426950408889634

    own = [
        pltpu.make_async_copy(seg_hbm, segs.at[0], in_sem.at[0]),
        pltpu.make_async_copy(k_hbm.at[0], k_raw, in_sem.at[1]),
        pltpu.make_async_copy(q_hbm.at[0], q_raw, in_sem.at[2]),
    ] + [
        pltpu.make_async_copy(
            v_hbm.at[0, :, pl.ds(h * HD, HD)], buf.at[0, HK + h], in_sem.at[3 + h]
        )
        for h in range(HK)
    ]
    for copy in own:
        copy.start()
    for j in range(1, NBACK + 1):
        segs[j] = jnp.full((1, ROWS), -1, jnp.int32)

    barrier = pltpu.get_barrier_semaphore()
    for k in range(1, 16):
        pl.semaphore_signal(
            barrier, inc=1, device_id={"ctx": lax.rem(d + k, 16)}, device_id_type=MESH
        )
    own[0].wait()
    for h in range(HK):
        own[3 + h].wait()
    pl.semaphore_wait(barrier, 15)

    def copy_to(src_slot, dst_slot, target, sem, t):
        return pltpu.make_async_remote_copy(
            buf.at[src_slot, t], buf.at[dst_slot, t], sem, recv_sem.at[dst_slot, t],
            device_id={"ctx": target}, device_id_type=MESH,
        )

    def ring(step):
        return col * 8 + lax.rem(y + step, 4) * 2 + core

    across = lax.rem(d + 8, 16)

    def y_copy(src_slot, step, t):
        return copy_to(src_slot, 2 * step, ring(step), y_send.at[step // 2], t)

    def x_copy(t):
        return copy_to(0, 8, across, x_send.at[0], t)

    def relay_up(t):
        return copy_to(2, 4, ring(1), r_send.at[0], t)

    def relay_down(t):
        return copy_to(6, 4, ring(3), r_send.at[0], t)

    def direct_far(t):
        return copy_to(0, 4, ring(2), f_send.at[0], t)

    def park(t):
        return copy_to(0, SPARE, ring(2), f_send.at[0], t)

    def cross_spare(t):
        return copy_to(SPARE, 4, across, s_send.at[0], t)

    def cross_park(t):
        return copy_to(2, SPARE, across, s_send.at[0], t)

    def wrap_spare(t):
        return copy_to(SPARE, 4, ring(1), s_send.at[0], t)

    def d_copy(k, t):
        return copy_to(2 * k, 2 * k + 1 - 2 * core, sibling, d_send.at[k], t)

    def d_copy_own(t):
        return copy_to(0, 1, sibling, d_send.at[0], t)

    def seg_copy(j):
        return pltpu.make_async_remote_copy(
            segs.at[0], segs.at[j], seg_send.at[j], seg_recv.at[j],
            device_id={"ctx": lax.rem(d + j, 16)}, device_id_type=MESH,
        )

    def send_own(t):
        for step in (1, 3):
            @pl.when(y + step < 4)
            def _():
                y_copy(0, step, t).start()

        @pl.when(col == 0)
        def _():
            x_copy(t).start()

        @pl.when(core == 0)
        def _():
            d_copy_own(t).start()

    def send_parked(kind):
        for h in range(HK):
            @pl.when((col == 0) & (y == (2 if h < 2 else 3)))
            def _():
                park(kind + h).start()

    def send_direct(where):
        @pl.when((y == 1) & (col == where))
        def _():
            for h in (2, 3):
                direct_far(HK + h).start()
                direct_far(h).start()

    for j in range(1, NBACK + 1):
        @pl.when(d + j < 16)
        def _():
            seg_copy(j).start()

    for h in range(HK):
        send_own(HK + h)
    send_parked(HK)

    own[1].wait()
    for h in range(HK):
        k_t[h] = k_raw[:, h * HD : (h + 1) * HD].T
    own[2].wait()

    def turn(n, carry):
        q_t[n] = q_raw[:, pl.ds(pl.multiple_of(n * HD, HD), HD)].T
        return carry

    lax.fori_loop(0, HQ, turn, 0, unroll=4)
    doc = lax.broadcasted_iota(jnp.int32, (HD, ROWS), 0)
    e_buf[...] = jnp.where(doc == segs[0], 1.0, 0.0).astype(jnp.bfloat16)

    lane = lax.broadcasted_iota(jnp.int32, (1, ROWS), 1).astype(jnp.float32)
    seg_f = segs[0].astype(jnp.float32)
    first = jnp.min(seg_f, axis=1, keepdims=True)
    start = jnp.zeros((1, ROWS), jnp.float32)
    for s in range(1, 8):
        before = jnp.sum(jnp.where(seg_f < float(s), 1.0, 0.0), axis=1, keepdims=True)
        start += jnp.where(seg_f == float(s), before, 0.0)
    local_pos[...] = lane - start
    first_doc[...] = jnp.broadcast_to(first, (1, ROWS))
    freq_index = lax.broadcasted_iota(jnp.int32, (HALF, ROWS), 0).astype(jnp.float32)
    cos_buf[...] = jnp.exp(-jnp.log(jnp.float32(THETA)) * 2.0 * freq_index / HD)

    for j in range(1, NBACK + 1):
        @pl.when(d >= j)
        def _():
            seg_copy(j).wait_recv()
    same = jnp.zeros((1, ROWS), jnp.float32)
    for j in range(1, NBACK + 1):
        same += jnp.where(segs[j].astype(jnp.float32) == first_doc[...], 1.0, 0.0)
    carried = jnp.sum(same, axis=1, keepdims=True)
    in_first = segs[0].astype(jnp.float32) == first_doc[...]
    pos = local_pos[...] + jnp.where(in_first, carried, 0.0)
    cos, sin = cos_sin(pos * cos_buf[...])
    cos_buf[...] = cos
    sin_buf[...] = sin

    for h in range(HK):
        buf[0, h] = rotated(k_t[h], cos, sin).T

    def build_mask(j, carry):
        m_t = jnp.where(doc == segs[j], 0.0, -DEAD).astype(jnp.bfloat16)
        m_buf[j] = m_t.T
        return carry

    lax.fori_loop(0, 2, build_mask, 0)
    for h in range(HK):
        send_own(h)
    send_parked(0)
    lax.fori_loop(2, NBACK + 1, build_mask, 0, unroll=7)

    def wait_in(slot, t):
        pltpu.make_async_remote_copy(
            buf.at[slot, t], buf.at[slot, t], d_send.at[0], recv_sem.at[slot, t],
            device_id={"ctx": sibling}, device_id_type=MESH,
        ).wait_recv()

    def serve(k, h, kind):
        t = h + kind

        @pl.when(chip >= k)
        def _():
            wait_in(2 * k, t)
            if k == 4:
                for step in (1, 3):
                    @pl.when(y + step >= 4)
                    def _():
                        y_copy(8, step, t).start()

                @pl.when(core == 1)
                def _():
                    d_copy(k, t).start()
                return
            if k == 1:
                @pl.when((h >= 2) & (col == 0) & (y == 3))
                def _():
                    cross_park(t).start()
            d_copy(k, t).start()

    def relay():
        for h in range(HK):
            for t in (HK + h, h):
                if h < 2:
                    @pl.when((chip >= 1) & (y < 3))
                    def _():
                        relay_up(t).start()
                else:
                    @pl.when(y == 3)
                    def _():
                        relay_down(t).start()

    def serve_spare(h, kind):
        t = h + kind

        @pl.when((col == 0) & (y == jnp.where(h < 2, 0, 1)))
        def _():
            wait_in(SPARE, t)
            cross_spare(t).start()

        @pl.when((col == 1) & (y == 3) & (h >= 2))
        def _():
            wait_in(SPARE, t)
            wrap_spare(t).start()

    def pipeline(stages, ahead=None):
        def scores(i):
            slots, h, g, is_own = stages[i]
            n = h * GROUP + g
            quer = jnp.concatenate([q_t[n], e_buf[...]], axis=0)
            peak = None if is_own else top[n]
            for a, slot in enumerate(slots):
                keys = jnp.concatenate([buf[slot, h], m_buf[slot]], axis=1)
                s = jnp.dot(keys, quer, preferred_element_type=jnp.float32)
                if is_own and a == 0:
                    later = lax.broadcasted_iota(jnp.int32, (ROWS, ROWS), 0) > (
                        lax.broadcasted_iota(jnp.int32, (ROWS, ROWS), 1)
                    )
                    s = jnp.where(later, -DEAD, s)
                s_buf[i % 2][pl.ds(a * ROWS, ROWS)] = s
                high = jnp.max(s, axis=0, keepdims=True)
                peak = high if peak is None else jnp.maximum(peak, high)
            return peak

        def weigh(i, peak):
            slots, h, g, is_own = stages[i]
            n = h * GROUP + g
            fade = None if is_own else jnp.exp2((top[n] - peak) * scale)
            top[n] = peak
            for a in range(len(slots)):
                p = jnp.exp2((s_buf[i % 2][pl.ds(a * ROWS, ROWS)] - peak) * scale)
                p_buf[i % 2][pl.ds(a * ROWS, ROWS)] = p.astype(jnp.bfloat16)
            return fade

        def add_up(i, fade):
            slots, h, g, is_own = stages[i]
            n = h * GROUP + g
            width = len(slots) * ROWS
            vals = jnp.concatenate([buf[slot, HK + h].T for slot in slots], axis=1)
            vals = jnp.concatenate([vals, jnp.ones((16, width), jnp.bfloat16)], axis=0)
            o = jnp.dot(vals, p_buf[i % 2][pl.ds(0, width)], preferred_element_type=jnp.float32)
            if is_own:
                acc[n] = o[:HD]
                total[n] = o[HD : HD + 1]
            else:
                acc[n] = acc[n] * fade + o[:HD]
                total[n] = total[n] * fade + o[HD : HD + 1]

        peaks, fades = {}, {}
        for i in range(len(stages) + 2):
            if ahead is not None and i < len(stages) and i % GROUP == 0:
                ahead(i // GROUP)
            if i < len(stages):
                peaks[i] = scores(i)
            if i >= 2:
                add_up(i - 2, fades[i - 2])
            if 1 <= i <= len(stages):
                fades[i - 1] = weigh(i - 1, peaks[i - 1])

    def heads(slots, h, is_own=False):
        return [(slots, h, g, is_own) for g in range(GROUP)]

    def wait_both(slot, h):
        wait_in(slot, HK + h)
        wait_in(slot, h)

    def spin(h):
        for g in range(GROUP):
            n = h * GROUP + g
            q_t[n] = rotated(q_t[n], cos_buf[...], sin_buf[...])

    def own_step(i, carry):
        h = 2 * i
        spin(h)
        spin(h + 1)

        def ahead(part):
            if part == 1:
                serve(4, h + 1, HK)

        @pl.when(i == 0)
        def _():
            serve(4, 0, HK)

        @pl.when(core == 0)
        def _():
            pipeline(heads([0], h, True) + heads([0], h + 1, True), ahead)

        @pl.when(core == 1)
        def _():
            wait_both(1, h)
            wait_both(1, h + 1)
            pipeline(heads([0, 1], h, True) + heads([0, 1], h + 1, True), ahead)

        @pl.when(i == 0)
        def _():
            serve(4, 2, HK)

        return carry

    def serve_sides(h, kind):
        serve(1, h, kind)
        serve(3, h, kind)

    lax.fori_loop(0, HK // 2, own_step, 0)
    serve(4, 0, 0)

    def take(part):
        if part > 0:
            serve(4, part, 0)
        if part == 1:
            serve_sides(0, HK)
            serve_sides(1, HK)
        if part == 2:
            serve_sides(2, HK)
        if part == 3:
            send_direct(1)
            serve_sides(3, HK)
            serve_sides(0, 0)

    @pl.when((col == 1) & (core == 0))
    def _():
        def ahead(part):
            take(part)
            wait_both(7, part)

        pipeline(sum([heads([8, 7], h) for h in range(HK)], []), ahead)

    @pl.when((col == 1) & (core == 1))
    def _():
        pipeline(sum([heads([8], h) for h in range(HK)], []), take)

    @pl.when(col == 0)
    def _():
        for part in range(HK):
            take(part)

    serve_sides(1, 0)

    def near_step(i, carry):
        h = 2 * i

        def between(part):
            @pl.when((i == 0) & (part == 1))
            def _():
                serve_sides(2, 0)
                serve_sides(3, 0)
                send_direct(0)
                relay()
                for u in range(HK):
                    serve_spare(u, HK)

            if part == 3:
                @pl.when(i == 0)
                def _():
                    for u in range(HK):
                        serve_spare(u, 0)

                @pl.when((i == 1) & (col == 1))
                def _():
                    serve(2, 0, HK)
                    serve(2, 0, 0)

        slots = [2 * k - 1 + 2 * core for k in (1, 3)]

        @pl.when(col == 1)
        def _():
            def ahead(part):
                between(part)
                wait_both(slots[part % 2], h + part // 2)

            stages = []
            for u in (h, h + 1):
                stages += heads([2, slots[0]], u) + heads([6, slots[1]], u)
            pipeline(stages, ahead)

        @pl.when(col == 0)
        def _():
            between(1)
            between(3)

            def small(u, inner):
                k = 2 * lax.rem(u, 2) + 1

                @pl.when(chip >= k)
                def _():
                    slot = 2 * k - 1 + 2 * core
                    wait_both(slot, h + lax.div(u, 2))
                    pipeline(heads([2 * k, slot], h + lax.div(u, 2)))
                return inner

            lax.fori_loop(0, 4, small, 0)

            @pl.when(i == 1)
            def _():
                serve(2, 0, HK)
                serve(2, 0, 0)

        return carry

    lax.fori_loop(0, HK // 2, near_step, 0)

    @pl.when(chip >= 2)
    def _():
        slot = 3 + 2 * core

        def ahead(part):
            if part < 3:
                serve(2, part + 1, HK)
                serve(2, part + 1, 0)
            wait_both(slot, part)

        pipeline(sum([heads([4, slot], h) for h in range(HK)], []), ahead)

    for j in range(1, NBACK + 1):
        @pl.when(d + j < 16)
        def _():
            seg_copy(j).wait_send()

    def drain(sem, chunks):
        ref = buf.at[0, pl.ds(0, chunks)]
        pltpu.make_async_remote_copy(
            ref, ref, sem, recv_sem.at[0, 0], device_id={"ctx": sibling}, device_id_type=MESH
        ).wait_send()

    for step in (1, 3):
        @pl.when((col == 1) | (y + step < 4))
        def _():
            drain(y_send.at[step // 2], 2 * HK)

    @pl.when(col == 0)
    def _():
        drain(x_send.at[0], 2 * HK)

    @pl.when((chip >= 1) | (y == 3))
    def _():
        drain(r_send.at[0], HK)

    @pl.when((y == 1) | ((col == 0) & (y >= 2)))
    def _():
        drain(f_send.at[0], HK)

    @pl.when((y == 3) | ((col == 0) & (y < 2)))
    def _():
        drain(s_send.at[0], HK)

    @pl.when(core == 0)
    def _():
        drain(d_send.at[0], 2 * HK)

    for k in (1, 2, 3):
        @pl.when(chip >= k)
        def _():
            drain(d_send.at[k], 2 * HK)

    @pl.when((col == 1) & (core == 1))
    def _():
        drain(d_send.at[4], 2 * HK)


def finish(acc, total, out):
    for g in range(GROUP):
        o = (acc[g] / total[g]).astype(jnp.bfloat16)
        out[0, :, g * HD : (g + 1) * HD] = o.T


def body(queries, keys, values, segments):
    hbm = pl.BlockSpec(memory_space=pltpu.HBM)
    acc, total = pl.pallas_call(
        kernel,
        out_shape=(
            jax.ShapeDtypeStruct((HQ, HD, ROWS), jnp.float32),
            jax.ShapeDtypeStruct((HQ, 1, ROWS), jnp.float32),
        ),
        in_specs=[hbm] * 4,
        out_specs=(pl.BlockSpec(memory_space=pltpu.VMEM),) * 2,
        scratch_shapes=[
            pltpu.VMEM((ROWS, HQ * HD), jnp.bfloat16),
            pltpu.VMEM((ROWS, HK * HD), jnp.bfloat16),
            pltpu.VMEM((HK, HD, ROWS), jnp.bfloat16),
            pltpu.VMEM((NBACK + 2, 2 * HK, ROWS, HD), jnp.bfloat16),
            pltpu.VMEM((NBACK + 1, 1, ROWS), jnp.int32),
            pltpu.VMEM((HQ, HD, ROWS), jnp.bfloat16),
            pltpu.VMEM((NBACK + 1, ROWS, HD), jnp.bfloat16),
            pltpu.VMEM((HD, ROWS), jnp.bfloat16),
            pltpu.VMEM((HALF, ROWS), jnp.float32),
            pltpu.VMEM((HALF, ROWS), jnp.float32),
            pltpu.VMEM((HQ, 1, ROWS), jnp.float32),
            pltpu.VMEM((2 * ROWS, ROWS), jnp.float32),
            pltpu.VMEM((2 * ROWS, ROWS), jnp.float32),
            pltpu.VMEM((2 * ROWS, ROWS), jnp.bfloat16),
            pltpu.VMEM((2 * ROWS, ROWS), jnp.bfloat16),
            pltpu.VMEM((1, ROWS), jnp.float32),
            pltpu.VMEM((1, ROWS), jnp.float32),
            pltpu.SemaphoreType.DMA((7,)),
            pltpu.SemaphoreType.DMA((NBACK + 2, 2 * HK)),
            pltpu.SemaphoreType.DMA((NBACK + 1,)),
            pltpu.SemaphoreType.DMA((NBACK + 1,)),
            pltpu.SemaphoreType.DMA((2,)),
            pltpu.SemaphoreType.DMA((1,)),
            pltpu.SemaphoreType.DMA((5,)),
            pltpu.SemaphoreType.DMA((1,)),
            pltpu.SemaphoreType.DMA((1,)),
            pltpu.SemaphoreType.DMA((1,)),
        ],
        compiler_params=pltpu.CompilerParams(collective_id=0, has_side_effects=True, vmem_limit_bytes=VLIM),
    )(*(pltpu.with_memory_space_constraint(x, pltpu.HBM) for x in (queries, keys, values, segments)))
    return pl.pallas_call(
        finish,
        grid=(HK,),
        out_shape=jax.ShapeDtypeStruct((1, ROWS, HQ * HD), jnp.bfloat16),
        in_specs=[
            pl.BlockSpec((GROUP, HD, ROWS), lambda h: (h, 0, 0)),
            pl.BlockSpec((GROUP, 1, ROWS), lambda h: (h, 0, 0)),
        ],
        out_specs=pl.BlockSpec((1, ROWS, GROUP * HD), lambda h: (0, 0, h)),
        compiler_params=pltpu.CompilerParams(vmem_limit_bytes=8 << 20),
    )(acc, total)


def solution(mesh):
    placed = (P("dp", "ctx", None), P("dp", "ctx", None), P("dp", "ctx", None), P("dp", "ctx"))
    return jax.shard_map(
        body, mesh=mesh, in_specs=placed, out_specs=P("dp", "ctx", None), check_vma=False
    )
```
